8 devices in a mesh: rep: 1 (over z), tp: 2 (over y), ep: 4 (over x, core).
Axes of the slice: x: 2, y: 2, z: 1, core: 2. Of those that a mesh axis runs over, the one named last changes fastest.
Arguments:
- hidden: bfloat16 [1024, 1024], P(('rep', 'ep'))
- g_norm: float32 [1024], replicated
- w_q: bfloat16 [1024, 1024], P(None, 'tp')
- w_k: bfloat16 [1024, 512], P(None, 'tp')
- w_v: bfloat16 [1024, 512], P(None, 'tp')
- w_o: bfloat16 [1024, 1024], P('tp')
- k_cache: bfloat16 [1024, 256, 8, 64], P(('rep', 'ep'), None, 'tp')
- v_cache: bfloat16 [1024, 256, 8, 64], P(('rep', 'ep'), None, 'tp')
- lengths: int32 [1024], P(('rep', 'ep'))
- w_sh_gate: bfloat16 [1024, 512], P(None, 'tp')
- w_sh_up: bfloat16 [1024, 512], P(None, 'tp')
- w_sh_down: bfloat16 [512, 1024], P('tp')
- w_gate: bfloat16 [32, 1024, 512], P(('ep', 'tp'))
- w_up: bfloat16 [32, 1024, 512], P(('ep', 'tp'))
- w_down: bfloat16 [32, 512, 1024], P(('ep', 'tp'))
- expert_ids: int32 [1024, 8], P(('rep', 'ep'))
- gate_vals: float32 [1024, 8], P(('rep', 'ep'))
Outputs:
- output: bfloat16 [1024, 1024], P(('rep', 'ep'))
All inputs are finite; a program needn't handle non-finite values.
Results may differ from the reference program's by a relative error of at most 0.00409599.
Values are sent between devices in bfloat16 or wider.
A program may use at most 1 GiB of HBM per device.

```python
import math
import jax
import jax.numpy as jnp
from jax import lax

D = 1024
HEADS = 16
KV_HEADS = 8
HEAD = 64
EXPERTS = 32
TOP = 8
FF = 512
FS = 512
B = 256
S = 256
EP = 4
TP = 2
RMS_EPS = 1e-6
N_TOK = EP * B
N_DEVICES = EP * TP
LOCAL_EXP = EXPERTS // N_DEVICES
CAP = min(B, 2 * B * TOP // N_DEVICES)
MAX_ROWS = min(N_TOK, EP * CAP)


def draw_routing(route_key):
    avg_load = B * TOP // N_DEVICES
    spread = CAP - avg_load

    def one_shard(shard_key):
        key_pair, key_delta, key_tok, key_local = jax.random.split(shard_key, 4)
        pair_perm = jax.random.permutation(key_pair, N_DEVICES)
        deltas = jax.random.randint(key_delta, (N_DEVICES // 2,), 0, spread + 1).at[0].set(spread)
        change = jnp.zeros((N_DEVICES,), jnp.int32).at[pair_perm[0::2]].add(deltas).at[pair_perm[1::2]].add(-deltas)
        bounds = jnp.cumsum(avg_load + change)
        dev_list = jnp.searchsorted(bounds, jnp.arange(B * TOP), side='right').astype(jnp.int32)
        dev_grid = dev_list.reshape(TOP, B).T[jax.random.permutation(key_tok, B)]
        local_ids = jax.random.randint(key_local, (B, TOP), 0, LOCAL_EXP)
        return (dev_grid * LOCAL_EXP + local_ids).astype(jnp.int32)

    return jax.vmap(one_shard)(jax.random.split(route_key, EP)).reshape(N_TOK, TOP)


def setup_inputs(seed: int = 0, part: int = 0) -> dict:
    base_key = jax.random.key(seed)
    part_key = jax.random.fold_in(base_key, part)
    shared = jax.random.split(base_key, 12)
    own = jax.random.split(part_key, 6)

    def normal(rkey, shape, scale):
        return (jax.random.normal(rkey, shape, jnp.float32) * scale).astype(jnp.bfloat16)

    hidden = normal(own[0], (N_TOK, D), 1.0)
    k_cache = normal(own[1], (N_TOK, S, KV_HEADS, HEAD), 1.0)
    v_cache = normal(own[2], (N_TOK, S, KV_HEADS, HEAD), 1.0)
    lengths = jax.random.randint(own[3], (N_TOK,), S // 8, S + 1).at[0].set(S).at[1].set(S // 8).astype(jnp.int32)
    expert_ids = draw_routing(own[4])
    raw_gate = jax.random.uniform(own[5], (N_TOK, TOP), jnp.float32, 0.1, 1.0)
    gate_vals = 1.5 * raw_gate / jnp.sqrt(jnp.sum(raw_gate * raw_gate, axis=1, keepdims=True))
    g_norm = jax.random.uniform(shared[0], (D,), jnp.float32, 0.5, 1.5)
    w_q = normal(shared[1], (D, HEADS * HEAD), D ** -0.5)
    w_k = normal(shared[2], (D, KV_HEADS * HEAD), D ** -0.5)
    w_v = normal(shared[3], (D, KV_HEADS * HEAD), D ** -0.5)
    w_o = normal(shared[4], (HEADS * HEAD, D), 0.5 * math.sqrt(S) * (HEADS * HEAD) ** -0.5)
    w_sh_gate = normal(shared[5], (D, FS), D ** -0.5)
    w_sh_up = normal(shared[6], (D, FS), D ** -0.5)
    w_sh_down = normal(shared[7], (FS, D), FS ** -0.5)
    w_gate = normal(shared[8], (EXPERTS, D, FF), D ** -0.5)
    w_up = normal(shared[9], (EXPERTS, D, FF), D ** -0.5)
    w_down = normal(shared[10], (EXPERTS, FF, D), FF ** -0.5)
    return {'hidden': hidden, 'g_norm': g_norm, 'w_q': w_q, 'w_k': w_k, 'w_v': w_v, 'w_o': w_o, 'k_cache': k_cache, 'v_cache': v_cache, 'lengths': lengths, 'w_sh_gate': w_sh_gate, 'w_sh_up': w_sh_up, 'w_sh_down': w_sh_down, 'w_gate': w_gate, 'w_up': w_up, 'w_down': w_down, 'expert_ids': expert_ids, 'gate_vals': gate_vals}


def rms_norm(hidden, g_norm):
    hid32 = hidden.astype(jnp.float32)
    inv_rms = lax.rsqrt(jnp.mean(hid32 * hid32, axis=-1, keepdims=True) + RMS_EPS)
    return (hid32 * inv_rms * g_norm).astype(jnp.bfloat16)


def swiglu(x_rows, w_in_gate, w_in_up, w_out):
    gate_a = jnp.dot(x_rows, w_in_gate, preferred_element_type=jnp.float32)
    up_b = jnp.dot(x_rows, w_in_up, preferred_element_type=jnp.float32)
    act_bf = (jax.nn.silu(gate_a) * up_b).astype(jnp.bfloat16)
    return jnp.dot(act_bf, w_out, preferred_element_type=jnp.float32)


def attend_token(operands):
    q_tok, k_tok, v_tok, k_self, v_self, length = operands
    q_grp = q_tok.astype(jnp.float32).reshape(KV_HEADS, HEADS // KV_HEADS, HEAD)
    inv_sqrt = HEAD ** -0.5
    scores = jnp.einsum('kgd,skd->kgs', q_grp, k_tok.astype(jnp.float32)) * inv_sqrt
    scores = jnp.where(jnp.arange(S) < length, scores, -1e30)
    self_score = jnp.einsum('kgd,kd->kg', q_grp, k_self.astype(jnp.float32)) * inv_sqrt
    row_peak = jnp.maximum(jnp.max(scores, axis=-1), self_score)
    probs_f32 = jnp.exp(scores - row_peak[:, :, None])
    self_prob = jnp.exp(self_score - row_peak)
    prob_sum = jnp.sum(probs_f32, axis=-1) + self_prob
    probs_bf = (probs_f32 / prob_sum[:, :, None]).astype(jnp.bfloat16).astype(jnp.float32)
    self_bf = (self_prob / prob_sum).astype(jnp.bfloat16).astype(jnp.float32)
    context = jnp.einsum('kgs,skd->kgd', probs_bf, v_tok.astype(jnp.float32))
    context = context + self_bf[:, :, None] * v_self.astype(jnp.float32)[:, None, :]
    return context.astype(jnp.bfloat16).reshape(HEADS * HEAD)


def reference(hidden, g_norm, w_q, w_k, w_v, w_o, k_cache, v_cache, lengths, w_sh_gate, w_sh_up, w_sh_down, w_gate, w_up, w_down, expert_ids, gate_vals):
    x_rows = rms_norm(hidden, g_norm)
    q_all = jnp.dot(x_rows, w_q, preferred_element_type=jnp.float32).astype(jnp.bfloat16).reshape(N_TOK, HEADS, HEAD)
    k_new = jnp.dot(x_rows, w_k, preferred_element_type=jnp.float32).astype(jnp.bfloat16).reshape(N_TOK, KV_HEADS, HEAD)
    v_new = jnp.dot(x_rows, w_v, preferred_element_type=jnp.float32).astype(jnp.bfloat16).reshape(N_TOK, KV_HEADS, HEAD)
    context = lax.map(attend_token, (q_all, k_cache, v_cache, k_new, v_new, lengths))
    attn = jnp.dot(context, w_o, preferred_element_type=jnp.float32)
    shared_out = swiglu(x_rows, w_sh_gate, w_sh_up, w_sh_down)
    flat_ids = expert_ids.reshape(-1)
    sort_order = jnp.argsort(flat_ids, stable=True)
    counts = jax.ops.segment_sum(jnp.ones_like(flat_ids), flat_ids, num_segments=EXPERTS)
    starts = jnp.cumsum(counts) - counts
    tok_pad = jnp.concatenate([sort_order // TOP, jnp.zeros((MAX_ROWS,), jnp.int32)])
    gate_pad = jnp.concatenate([gate_vals.reshape(-1)[sort_order], jnp.zeros((MAX_ROWS,), jnp.float32)])

    def expert_step(routed, operands):
        w_in_gate, w_in_up, w_out, start, count = operands
        tok_win = lax.dynamic_slice(tok_pad, (start,), (MAX_ROWS,))
        gate_win = jnp.where(jnp.arange(MAX_ROWS) < count, lax.dynamic_slice(gate_pad, (start,), (MAX_ROWS,)), 0.0)
        expert_out = swiglu(x_rows[tok_win], w_in_gate, w_in_up, w_out).astype(jnp.bfloat16).astype(jnp.float32)
        return routed.at[tok_win].add(expert_out * gate_win[:, None]), None

    routed, _ = lax.scan(expert_step, jnp.zeros((N_TOK, D), jnp.float32), (w_gate, w_up, w_down, starts, counts))
    return (hidden.astype(jnp.float32) + attn + shared_out + routed).astype(jnp.bfloat16)
```

```python
import functools

import jax
import jax.numpy as jnp
from jax import lax
from jax.experimental import pallas as pl
from jax.experimental.pallas import tpu as pltpu
from jax.sharding import PartitionSpec as P

RMS_EPS = 1e-6
TB = 8
SLOTS = 4
ROWS = 128
LANES = 128
BF = jnp.bfloat16
F32 = jnp.float32


def one_hot_mat(rows, cols, fn):
    r = lax.broadcasted_iota(jnp.int32, (rows, cols), 0)
    c = lax.broadcasted_iota(jnp.int32, (rows, cols), 1)
    return jnp.where(fn(r, c), 1.0, 0.0).astype(BF)


def dotf(a, b):
    return jnp.dot(a, b, preferred_element_type=F32)


def dot_nt(a, b):
    return lax.dot_general(a, b, (((1,), (1,)), ((), ())), preferred_element_type=F32)


def layer_kernel(cfg, hid_hbm, gn_hbm, wq_hbm, wk_hbm, wv_hbm, wo_hbm, k_hbm, v_hbm, len_hbm, wsg_hbm, wsu_hbm, wsd_hbm,
                 wg_hbm, wu_hbm, wd_hbm, ids_hbm, gts_hbm, out_hbm,
                 hall, xall, gn, wq, wk, wv, wo, wsg, wsu, wsd, wg, wu, wd, idg, gtg, gb, kbuf, vbuf, lens,
                 q0, q1, kn, vn, ctx, dense, part, rpf, rph, rx, tx, ry, act, outb,
                 lsem, wsem, ksem, vsem, osem, s_send, s_recv):
    n_rows, kvh, hd, seq, n_local, tp_size, ep_size = cfg
    d_model = hall.shape[2]
    n_chunk = n_rows // ROWS
    n_blk = n_rows // TB
    kd = kvh * hd
    half = ROWS // tp_size
    tp = lax.axis_index('tp')
    ep = lax.axis_index('ep')
    partner = {'ep': ep + 1 - 2 * lax.rem(ep, 2)}
    xnbr = {'ep': lax.rem(ep + ep_size // 2, ep_size)}
    ynbr = {'tp': 1 - tp}

    def local(src, dst, sem):
        return pltpu.make_async_copy(src, dst, sem)

    def remote(i, src, dst, dev):
        return pltpu.make_async_remote_copy(src_ref=src, dst_ref=dst, send_sem=s_send.at[i], recv_sem=s_recv.at[i],
                                            device_id=dev, device_id_type=pl.DeviceIdType.MESH)

    def rows(i):
        return pl.ds(i * ROWS, ROWS)

    hid_cp = [local(hid_hbm, hall.at[0], lsem.at[0])]
    small_cp = [local(ids_hbm, idg.at[0], lsem.at[1]), local(gts_hbm, gtg.at[0], lsem.at[2]),
                local(gn_hbm, gn, lsem.at[3]), local(len_hbm, lens, lsem.at[4])]
    qkv_cp = [local(wq_hbm, wq, lsem.at[5]), local(wk_hbm, wk, lsem.at[6]), local(wv_hbm, wv, lsem.at[7])]
    sh_cp = [local(wsg_hbm, wsg, lsem.at[8]), local(wsu_hbm, wsu, lsem.at[9]), local(wsd_hbm, wsd, lsem.at[10]),
             local(wo_hbm, wo, lsem.at[11])]
    exp_cp = [local(wg_hbm, wg, wsem.at[0]), local(wu_hbm, wu, wsem.at[1]), local(wd_hbm, wd, wsem.at[2])]

    def kv_cp(b, slot):
        at = pl.ds(b * TB, TB)
        return (local(k_hbm.at[at], kbuf.at[slot], ksem.at[slot]), local(v_hbm.at[at], vbuf.at[slot], vsem.at[slot]))

    for c in hid_cp + small_cp + qkv_cp:
        c.start()
    for b in range(SLOTS):
        for c in kv_cp(b, b):
            c.start()
    for c in exp_cp + sh_cp:
        c.start()

    barrier = pltpu.get_barrier_semaphore()
    for dev in (partner, xnbr, ynbr):
        pl.semaphore_signal(barrier, inc=1, device_id=dev, device_id_type=pl.DeviceIdType.MESH)
    pl.semaphore_wait(barrier, 3)

    x_hid = [remote(i, hall.at[0, rows(i)], hall.at[2, rows(i)], xnbr) for i in range(n_chunk)]
    p_hid = [remote(2 + i, hall.at[0, rows(i)], hall.at[1, rows(i)], partner) for i in range(n_chunk)]
    f_hid = [remote(4 + i, hall.at[2, rows(i)], hall.at[3, rows(i)], partner) for i in range(n_chunk)]
    x_idg = [remote(6, idg.at[0], idg.at[2], xnbr), remote(7, gtg.at[0], gtg.at[2], xnbr)]
    p_idg = [remote(8, idg.at[0], idg.at[1], partner), remote(9, gtg.at[0], gtg.at[1], partner)]
    f_idg = [remote(10, idg.at[2], idg.at[3], partner), remote(11, gtg.at[2], gtg.at[3], partner)]
    c_far = [remote(12 + i, part.at[3, rows(i)], rpf.at[rows(i)], partner) for i in range(n_chunk)]
    x_ret = [remote(14 + i, part.at[2, rows(i)], rx.at[rows(i)], xnbr) for i in range(n_chunk)]
    c_near = [remote(16 + i, part.at[1, rows(i)], rph.at[rows(i)], partner) for i in range(n_chunk)]

    def mine(i):
        return pl.ds(pl.multiple_of(i * ROWS + tp * half, half), half)

    def theirs(i):
        return pl.ds(pl.multiple_of(i * ROWS + (1 - tp) * half, half), half)

    y_sum = [remote(18 + i, tx.at[i], ry.at[i], ynbr) for i in range(n_chunk)]
    y_out = [remote(20 + i, outb.at[mine(i)], outb.at[mine(i)], ynbr) for i in range(n_chunk)]

    for c in small_cp:
        c.wait()
    for c in x_idg + p_idg:
        c.start()
    for c in hid_cp:
        c.wait()
    for c in x_hid + p_hid:
        c.start()

    def normalize(grp, r0, n):
        def body(j, carry):
            at = pl.ds(pl.multiple_of(r0 + j * 32, 32), 32)
            h32 = hall[grp, at, :].astype(F32)
            inv = lax.rsqrt(jnp.mean(h32 * h32, axis=-1, keepdims=True) + RMS_EPS)
            xall[grp, at, :] = (h32 * inv * gn[...]).astype(BF)
            return carry
        lax.fori_loop(0, n // 32, body, 0)

    first_exp = (ep * tp_size + tp) * n_local

    def gate_table(grp):
        ids = idg[grp]
        vals = gtg[grp]
        picked = [jnp.sum(jnp.where(ids == first_exp + e, vals, 0.0), axis=0, keepdims=True) for e in range(n_local)]
        table = jnp.concatenate(picked + [jnp.zeros((LANES - n_local, n_rows), F32)], axis=0)
        cols = jnp.transpose(table)
        for e in range(n_local):
            gb[grp, e] = jnp.broadcast_to(cols[:, e:e + 1], (n_rows, LANES))

    normalize(0, 0, n_rows)
    for c in qkv_cp:
        c.wait()

    nq = wq.shape[1]
    q_bf = [dotf(xall[0], wq[:, j * 256:(j + 1) * 256]).astype(BF) for j in range(nq // 256)]
    for g, ref in enumerate((q0, q1)):
        acc = None
        for j in range(nq // 256):
            def sel(r, c, j=j, g=g):
                rr = r + j * 256
                return ((rr // (2 * hd)) == (c // hd)) & ((rr % (2 * hd)) == g * hd + c % hd)
            term = dotf(q_bf[j], one_hot_mat(256, kd, sel))
            acc = term if acc is None else acc + term
        ref[...] = acc
    kn[...] = dotf(xall[0], wk[...]).astype(BF).astype(F32)
    vn[...] = dotf(xall[0], wv[...]).astype(BF).astype(F32)

    R = TB * 2 * kvh
    per_tok = 2 * kvh
    expand_q = one_hot_mat(R, 2 * TB, lambda r, c: c == ((r % per_tok) // kvh) * TB + r // per_tok)
    expand_n = one_hot_mat(R, TB, lambda r, c: c == r // per_tok)
    gather_o = one_hot_mat(2 * TB, R, lambda r, c: (c // per_tok == r % TB) & ((c % per_tok) // kvh == r // TB))
    rr = lax.broadcasted_iota(jnp.int32, (R, kd), 0)
    cc = lax.broadcasted_iota(jnp.int32, (R, kd), 1)
    own = (rr % kvh) == (cc // hd)
    pos = lax.broadcasted_iota(jnp.int32, (per_tok, seq), 1)
    scale = hd ** -0.5

    def attn_block(b, carry):
        slot = lax.rem(b, SLOTS)
        tok = pl.ds(pl.multiple_of(b * TB, TB), TB)
        kc, vc = kv_cp(b, slot)
        qq = jnp.concatenate([q0[tok, :], q1[tok, :]], axis=0).astype(BF)
        q_blk = jnp.where(own, dotf(expand_q, qq), 0.0)
        k_self = dotf(expand_n, kn[tok, :].astype(BF))
        v_self = dotf(expand_n, vn[tok, :].astype(BF))
        self_score = jnp.sum(q_blk * k_self, axis=-1, keepdims=True) * scale
        kc.wait()
        parts = []
        for t in range(TB):
            s_t = dotf(q_blk[t * per_tok:(t + 1) * per_tok].astype(BF), kbuf[slot, t])
            parts.append(jnp.where(pos < lens[b * TB + t], s_t * scale, -1e30))
        scores = jnp.concatenate(parts, axis=0)
        peak = jnp.maximum(jnp.max(scores, axis=-1, keepdims=True), self_score)
        prob = jnp.exp(scores - peak)
        self_prob = jnp.exp(self_score - peak)
        inv = 1.0 / (jnp.sum(prob, axis=-1, keepdims=True) + self_prob)
        prob = prob * inv
        self_bf = (self_prob * inv).astype(BF).astype(F32)
        vc.wait()
        outs = [dot_nt(prob[t * per_tok:(t + 1) * per_tok].astype(BF), vbuf[slot, t]) for t in range(TB)]
        o = jnp.concatenate(outs, axis=0) + self_bf * v_self
        o = jnp.where(own, o, 0.0).astype(BF)
        o2 = dotf(gather_o, o)
        ctx[tok, 0:kd] = o2[0:TB]
        ctx[tok, kd:2 * kd] = o2[TB:2 * TB]

        @pl.when(b + SLOTS < n_blk)
        def _():
            for c in kv_cp(b + SLOTS, slot):
                c.start()
        return carry

    def attend(lo, hi):
        lax.fori_loop(lo, hi, attn_block, 0)

    ff = wg.shape[2]

    def unit(grp, r0):
        at = pl.ds(r0, ROWS)

        def body(e, carry):
            xr = xall[grp, at, :]
            for j in range(ff // 256):
                cs = slice(j * 256, (j + 1) * 256)
                g_a = dotf(xr, wg[e, :, cs])
                u_b = dotf(xr, wu[e, :, cs])
                act[:, cs] = (g_a * jax.nn.sigmoid(g_a) * u_b).astype(BF)
            gate = gb[grp, e, at, :]
            hit = gate > 0.0
            first = e == 0
            for j in range(d_model // 256):
                y = dotf(act[...], wd[e, :, j * 256:(j + 1) * 256]).astype(BF).astype(F32)
                for m in range(256 // LANES):
                    ls = slice(j * 256 + m * LANES, j * 256 + (m + 1) * LANES)
                    add = jnp.where(hit, gate * y[:, m * LANES:(m + 1) * LANES], 0.0)
                    part[grp, at, ls] = jnp.where(first, add, part[grp, at, ls] + add)
            return carry

        lax.fori_loop(0, n_local, body, 0)

    splits = [n_blk * s // 32 for s in (0, 8, 13, 32)]
    attend(splits[0], splits[1])
    for c in x_idg + p_idg:
        c.wait_recv()
    for c in f_idg:
        c.start()
    x_hid[0].wait_recv()
    f_hid[0].start()
    gate_table(0)
    gate_table(1)
    gate_table(2)
    normalize(2, 0, ROWS)
    attend(splits[1], splits[2])
    for i in range(1, n_chunk):
        x_hid[i].wait_recv()
        f_hid[i].start()
        normalize(2, i * ROWS, ROWS)
    for c in f_idg:
        c.wait_recv()
    gate_table(3)
    for c in exp_cp:
        c.wait()
    for i in range(n_chunk):
        f_hid[i].wait_recv()
        normalize(3, i * ROWS, ROWS)
        unit(3, i * ROWS)
        c_far[i].start()
        unit(2, i * ROWS)
        c_far[i].wait_recv()
        at = rows(i)
        part[2, at, :] = part[2, at, :] + rpf[at, :]
        x_ret[i].start()
    for i in range(n_chunk):
        p_hid[i].wait_recv()
        normalize(1, i * ROWS, ROWS)
        unit(1, i * ROWS)
        c_near[i].start()
    for i in range(n_chunk):
        unit(0, i * ROWS)
    attend(splits[2], splits[3])

    for c in sh_cp:
        c.wait()
    swap = one_hot_mat(2 * kd, 2 * kd, lambda r, c: ((r // kd) == ((c // hd) % 2)) & ((r % kd) // hd == c // (2 * hd)) & (r % hd == c % hd))
    ctx_bf = dotf(ctx[...].astype(BF), swap).astype(BF)
    sg = dotf(xall[0], wsg[...])
    su = dotf(xall[0], wsu[...])
    sa = (sg * jax.nn.sigmoid(sg) * su).astype(BF)
    for j in range(d_model // 256):
        cs = slice(j * 256, (j + 1) * 256)
        dense[:, cs] = dotf(ctx_bf, wo[:, cs]) + dotf(sa, wsd[:, cs]) + part[0, :, cs]

    for i in range(n_chunk):
        c_near[i].wait_recv()
        x_ret[i].wait_recv()
        at = theirs(i)
        tx[i] = dense[at, :] + rph[at, :] + rx[at, :]
        y_sum[i].start()
    out_cp = []
    for i in range(n_chunk):
        y_sum[i].wait_recv()
        at = mine(i)
        outb[at, :] = (hall[0, at, :].astype(F32) + (dense[at, :] + rph[at, :] + rx[at, :] + ry[i])).astype(BF)
        y_out[i].start()
    for i in range(n_chunk):
        y_out[i].wait_recv()
        c = local(outb.at[rows(i)], out_hbm.at[rows(i)], osem.at[i])
        c.start()
        out_cp.append(c)
    for c in x_hid + p_hid + f_hid + x_idg + p_idg + f_idg + c_far + x_ret + c_near + y_sum + y_out:
        c.wait_send()
    for c in out_cp:
        c.wait()


def solution(mesh):
    tp_size = mesh.shape['tp']
    ep_size = mesh.shape['ep']
    tok_spec = P(('rep', 'ep'), None)
    col_spec = P(None, 'tp')
    row_spec = P('tp', None)
    cache_spec = P(('rep', 'ep'), None, 'tp', None)
    expert_spec = P(('ep', 'tp'), None, None)

    def device_step(hidden, g_norm, w_q, w_k, w_v, w_o, k_cache, v_cache, lengths, w_sh_gate, w_sh_up, w_sh_down, w_gate, w_up, w_down, expert_ids, gate_vals):
        n_rows, d = hidden.shape
        _, seq, kvh, hd = k_cache.shape
        n_local, _, ff = w_gate.shape
        fs = w_sh_gate.shape[1]
        kd = kvh * hd
        top = expert_ids.shape[1]
        k_t = k_cache.transpose(0, 2, 3, 1).reshape(n_rows, kd, seq)
        v_t = v_cache.transpose(0, 2, 3, 1).reshape(n_rows, kd, seq)
        cfg = (n_rows, kvh, hd, seq, n_local, tp_size, ep_size)
        half = ROWS // tp_size
        n_chunk = n_rows // ROWS
        args = (hidden, g_norm.reshape(1, d), w_q, w_k, w_v, w_o, k_t, v_t, lengths, w_sh_gate, w_sh_up, w_sh_down,
                w_gate, w_up, w_down, expert_ids.T, gate_vals.T)
        v = pltpu.VMEM
        dma = pltpu.SemaphoreType.DMA
        scratch = [
            v((4, n_rows, d), BF), v((4, n_rows, d), BF), v((1, d), F32), v(w_q.shape, BF), v(w_k.shape, BF), v(w_v.shape, BF), v(w_o.shape, BF),
            v(w_sh_gate.shape, BF), v(w_sh_up.shape, BF), v(w_sh_down.shape, BF), v(w_gate.shape, BF), v(w_up.shape, BF), v(w_down.shape, BF),
            v((4, top, n_rows), jnp.int32), v((4, top, n_rows), F32), v((4, n_local, n_rows, LANES), F32),
            v((SLOTS, TB, kd, seq), BF), v((SLOTS, TB, kd, seq), BF), pltpu.SMEM((n_rows,), jnp.int32),
            v((n_rows, kd), F32), v((n_rows, kd), F32), v((n_rows, kd), F32), v((n_rows, kd), F32), v((n_rows, 2 * kd), F32),
            v((n_rows, d), F32), v((4, n_rows, d), F32), v((n_rows, d), F32), v((n_rows, d), F32), v((n_rows, d), F32),
            v((n_chunk, half, d), F32), v((n_chunk, half, d), F32), v((ROWS, ff), BF), v((n_rows, d), BF),
            dma((12,)), dma((3,)), dma((SLOTS,)), dma((SLOTS,)), dma((n_chunk,)), dma((22,)), dma((22,)),
        ]
        return pl.pallas_call(
            functools.partial(layer_kernel, cfg),
            out_shape=jax.ShapeDtypeStruct((n_rows, d), BF),
            in_specs=[pl.BlockSpec(memory_space=pl.ANY)] * len(args),
            out_specs=pl.BlockSpec(memory_space=pl.ANY),
            scratch_shapes=scratch,
            compiler_params=pltpu.CompilerParams(collective_id=0, has_side_effects=True, vmem_limit_bytes=67043328),
            name='layer',
        )(*args)

    return jax.shard_map(device_step, mesh=mesh, in_specs=(tok_spec, P(None), col_spec, col_spec, col_spec, row_spec, cache_spec, cache_spec, P(('rep', 'ep')), col_spec, col_spec, row_spec, expert_spec, expert_spec, expert_spec, tok_spec, tok_spec), out_specs=tok_spec, check_vma=False)
```

```python
import functools

import jax
import jax.numpy as jnp
from jax import lax
from jax.experimental import pallas as pl
from jax.experimental.pallas import tpu as pltpu
from jax.sharding import PartitionSpec as P

RMS_EPS = 1e-6
TB = 8
SLOTS = 6
ROWS = 128
SUB = 64
LANES = 128
BF = jnp.bfloat16
F32 = jnp.float32


def one_hot_mat(rows, cols, fn):
    r = lax.broadcasted_iota(jnp.int32, (rows, cols), 0)
    c = lax.broadcasted_iota(jnp.int32, (rows, cols), 1)
    return jnp.where(fn(r, c), 1.0, 0.0).astype(BF)


def dotf(a, b):
    return jnp.dot(a, b, preferred_element_type=F32)


def dot_nt(a, b):
    return lax.dot_general(a, b, (((1,), (1,)), ((), ())), preferred_element_type=F32)


def layer_kernel(cfg, hid_hbm, gn_hbm, wq_hbm, wk_hbm, wv_hbm, wo_hbm, k_hbm, v_hbm, len_hbm, wsg_hbm, wsu_hbm, wsd_hbm,
                 wg_hbm, wu_hbm, wd_hbm, ids_hbm, gts_hbm, out_hbm,
                 hall, xall, gn, wq, wk, wv, wo, wsg, wsu, wsd, wg, wu, wd, idg, gtg, gb, kbuf, vbuf, lens,
                 q0, q1, kn, vn, ctx, dense, part, rpf, rph, act, outb, qs, ss, sc, ps, sp, tf, ryf, xs, rxf, ty, ryo,
                 lsem, wsem, ksem, vsem, osem, s_send, s_recv):
    n_rows, kvh, hd, seq, n_local, tp_size, ep_size = cfg
    d_model = hall.shape[2]
    n_chunk = n_rows // ROWS
    n_sub = n_rows // SUB
    per_chunk = ROWS // SUB
    n_blk = n_rows // TB
    kd = kvh * hd
    half = SUB // tp_size
    tp = lax.axis_index('tp')
    ep = lax.axis_index('ep')
    partner = {'ep': ep + 1 - 2 * lax.rem(ep, 2)}
    xnbr = {'ep': lax.rem(ep + ep_size // 2, ep_size)}
    ynbr = {'tp': 1 - tp}

    def local(src, dst, sem):
        return pltpu.make_async_copy(src, dst, sem)

    n_remote = [0]

    def remote(src, dst, dev):
        i = n_remote[0]
        n_remote[0] += 1
        return pltpu.make_async_remote_copy(src_ref=src, dst_ref=dst, send_sem=s_send.at[i], recv_sem=s_recv.at[i],
                                            device_id=dev, device_id_type=pl.DeviceIdType.MESH)

    def rows(i):
        return pl.ds(i * ROWS, ROWS)

    def mine(s):
        return pl.ds(pl.multiple_of(s * SUB + tp * half, half), half)

    def theirs(s):
        return pl.ds(pl.multiple_of(s * SUB + (1 - tp) * half, half), half)

    hid_cp = [local(hid_hbm, hall.at[0], lsem.at[0])]
    small_cp = [local(ids_hbm, idg.at[0], lsem.at[1]), local(gts_hbm, gtg.at[0], lsem.at[2]),
                local(gn_hbm, gn, lsem.at[3]), local(len_hbm, lens, lsem.at[4])]
    qkv_cp = [local(wq_hbm, wq, lsem.at[5]), local(wk_hbm, wk, lsem.at[6]), local(wv_hbm, wv, lsem.at[7])]
    sh_cp = [local(wsg_hbm, wsg, lsem.at[8]), local(wsu_hbm, wsu, lsem.at[9]), local(wsd_hbm, wsd, lsem.at[10]),
             local(wo_hbm, wo, lsem.at[11])]
    exp_cp = [local(wg_hbm, wg, wsem.at[0]), local(wu_hbm, wu, wsem.at[1]), local(wd_hbm, wd, wsem.at[2])]

    def k_cp(b):
        slot = lax.rem(b, SLOTS)
        return local(k_hbm.at[pl.ds(b * TB, TB)], kbuf.at[slot], ksem.at[slot])

    def v_cp(b):
        slot = lax.rem(b, SLOTS)
        return local(v_hbm.at[pl.ds(b * TB, TB)], vbuf.at[slot], vsem.at[slot])

    for c in hid_cp + small_cp + qkv_cp + exp_cp:
        c.start()
    for b in range(SLOTS):
        k_cp(b).start()
        v_cp(b).start()
    for c in sh_cp:
        c.start()

    barrier = pltpu.get_barrier_semaphore()
    for dev in (partner, xnbr, ynbr):
        pl.semaphore_signal(barrier, inc=1, device_id=dev, device_id_type=pl.DeviceIdType.MESH)
    pl.semaphore_wait(barrier, 3)

    chunks = range(n_chunk)
    subs = range(n_sub)
    x_hid = [remote(hall.at[0, rows(i)], hall.at[2, rows(i)], xnbr) for i in chunks]
    p_hid = [remote(hall.at[0, rows(i)], hall.at[1, rows(i)], partner) for i in chunks]
    f_hid = [remote(hall.at[2, rows(i)], hall.at[3, rows(i)], partner) for i in chunks]
    x_idg = [remote(idg.at[0], idg.at[2], xnbr), remote(gtg.at[0], gtg.at[2], xnbr)]
    p_idg = [remote(idg.at[0], idg.at[1], partner), remote(gtg.at[0], gtg.at[1], partner)]
    f_idg = [remote(idg.at[2], idg.at[3], partner), remote(gtg.at[2], gtg.at[3], partner)]
    c_far = [remote(part.at[3, rows(i)], rpf.at[rows(i)], partner) for i in chunks]
    c_near = [remote(part.at[1, rows(i)], rph.at[rows(i)], partner) for i in chunks]
    y_far = [remote(tf.at[s], ryf.at[s], ynbr) for s in subs]
    x_ret = [remote(xs.at[s], rxf.at[s], xnbr) for s in subs]
    y_own = [remote(ty.at[s], ryo.at[s], ynbr) for s in subs]
    y_out = [remote(outb.at[mine(s)], outb.at[mine(s)], ynbr) for s in subs]

    for c in small_cp:
        c.wait()
    for c in x_idg + p_idg:
        c.start()
    for c in hid_cp:
        c.wait()
    for c in x_hid + p_hid:
        c.start()

    def normalize(grp, r0, n):
        def body(j, carry):
            at = pl.ds(pl.multiple_of(r0 + j * 32, 32), 32)
            h32 = hall[grp, at, :].astype(F32)
            inv = lax.rsqrt(jnp.mean(h32 * h32, axis=-1, keepdims=True) + RMS_EPS)
            xall[grp, at, :] = (h32 * inv * gn[...]).astype(BF)
            return carry
        lax.fori_loop(0, n // 32, body, 0)

    first_exp = (ep * tp_size + tp) * n_local

    def gate_table(grp):
        ids = idg[grp]
        vals = gtg[grp]
        picked = [jnp.sum(jnp.where(ids == first_exp + e, vals, 0.0), axis=0, keepdims=True) for e in range(n_local)]
        table = jnp.concatenate(picked + [jnp.zeros((LANES - n_local, n_rows), F32)], axis=0)
        cols = jnp.transpose(table)
        for e in range(n_local):
            gb[grp, e] = jnp.broadcast_to(cols[:, e:e + 1], (n_rows, LANES))

    R = TB * 2 * kvh
    per_tok = 2 * kvh
    expand_q = one_hot_mat(R, 2 * TB, lambda r, c: c == ((r % per_tok) // kvh) * TB + r // per_tok)
    expand_n = one_hot_mat(R, TB, lambda r, c: c == r // per_tok)
    gather_o = one_hot_mat(2 * TB, R, lambda r, c: (c // per_tok == r % TB) & ((c % per_tok) // kvh == r // TB))
    rr = lax.broadcasted_iota(jnp.int32, (R, kd), 0)
    cc = lax.broadcasted_iota(jnp.int32, (R, kd), 1)
    own = (rr % kvh) == (cc // hd)
    pos = lax.broadcasted_iota(jnp.int32, (per_tok, seq), 1)
    scale = hd ** -0.5

    def toks(b):
        return pl.ds(pl.multiple_of(b * TB, TB), TB)

    def stage_q(b, p):
        tok = toks(b)
        qq = jnp.concatenate([q0[tok, :], q1[tok, :]], axis=0).astype(BF)
        qs[p] = jnp.where(own, dotf(expand_q, qq), 0.0)

    def heads(t):
        return slice(t * per_tok, (t + 1) * per_tok)

    def stage_kv(b, p, with_v=True, with_k=True):
        if with_k:
            k_slot = lax.rem(b, SLOTS)
            k_self = dotf(expand_n, kn[toks(b), :].astype(BF))
            ss[p] = jnp.broadcast_to(jnp.sum(qs[p] * k_self, axis=-1, keepdims=True) * scale, (R, LANES))
        if with_v:
            v_slot = lax.rem(b - 2, SLOTS)
            v_self = dotf(expand_n, vn[toks(b - 2), :].astype(BF))
        outs = []
        for t in range(TB):
            if with_k:
                s_t = dotf(qs[p, heads(t), :].astype(BF), kbuf[k_slot, t])
                sc[p, heads(t), :] = jnp.where(pos < lens[b * TB + t], s_t * scale, -1e30)
            if with_v:
                outs.append(dot_nt(ps[p, heads(t), :].astype(BF), vbuf[v_slot, t]))
        if with_v:
            o = jnp.concatenate(outs, axis=0) + jnp.concatenate([sp[p]] * (kd // LANES), axis=1) * v_self
            o2 = dotf(gather_o, jnp.where(own, o, 0.0).astype(BF))
            ctx[toks(b - 2), 0:kd] = o2[0:TB]
            ctx[toks(b - 2), kd:2 * kd] = o2[TB:2 * TB]

    def stage_s(p):
        scores = sc[p]
        self_score = ss[p, :, 0:1]
        peak = jnp.maximum(jnp.max(scores, axis=-1, keepdims=True), self_score)
        prob = jnp.exp(scores - peak)
        self_prob = jnp.exp(self_score - peak)
        inv = 1.0 / (jnp.sum(prob, axis=-1, keepdims=True) + self_prob)
        ps[p] = prob * inv
        sp[p] = jnp.broadcast_to((self_prob * inv).astype(BF).astype(F32), (R, LANES))

    def attn_pair(j, carry):
        b = 2 * j
        for p in range(2):
            k_cp(b + p).wait()
            v_cp(b + p - 2).wait()
        for p in range(2):
            stage_kv(b + p, p)
            stage_s(1 - p)
            stage_q(jnp.minimum(b + p + 1, n_blk - 1), 1 - p)
        for p in range(2):
            @pl.when(b + p + SLOTS < n_blk)
            def _():
                k_cp(b + p + SLOTS).start()

            @pl.when(b + p - 2 + SLOTS < n_blk)
            def _():
                v_cp(b + p - 2 + SLOTS).start()
        return carry

    done = [0]

    def attend(hi):
        lo = done[0]
        done[0] = hi
        if lo == 0:
            for p in range(2):
                k_cp(p).wait()
                stage_q(p, p)
            for p in range(2):
                stage_kv(p, p, with_v=False)
            stage_s(0)
            stage_q(2, 0)
            for p in range(2):
                k_cp(p + SLOTS).start()
            lo = 2
        lax.fori_loop(lo // 2, hi // 2, attn_pair, 0)
        if hi == n_blk:
            for p in range(2):
                v_cp(n_blk - 2 + p).wait()
            stage_kv(n_blk, 0, with_k=False)
            stage_s(1)
            stage_kv(n_blk + 1, 1, with_k=False)

    ff = wg.shape[2]

    def unit(g0, i):
        at = rows(i)
        m2 = 2 * ROWS

        def body(e, carry):
            xr = xall[g0:g0 + 2, at, :].reshape(m2, d_model)
            for j in range(ff // 256):
                cs = slice(j * 256, (j + 1) * 256)
                g_a = dotf(xr, wg[e, :, cs])
                u_b = dotf(xr, wu[e, :, cs])
                act[:, cs] = (g_a * jax.nn.sigmoid(g_a) * u_b).astype(BF)
            gate = gb[g0:g0 + 2, e, at, :].reshape(m2, LANES)
            hit = gate > 0.0
            first = e == 0
            for j in range(d_model // 256):
                y = dotf(act[...], wd[e, :, j * 256:(j + 1) * 256]).astype(BF).astype(F32)
                for m in range(256 // LANES):
                    ls = slice(j * 256 + m * LANES, j * 256 + (m + 1) * LANES)
                    add = jnp.where(hit, gate * y[:, m * LANES:(m + 1) * LANES], 0.0).reshape(2, ROWS, LANES)
                    part[g0:g0 + 2, at, ls] = jnp.where(first, add, part[g0:g0 + 2, at, ls] + add)
            return carry

        lax.fori_loop(0, n_local, body, 0)

    def sub_of(i):
        return range(i * per_chunk, (i + 1) * per_chunk)

    def far_y(i):
        c_far[i].wait_recv()
        for s in sub_of(i):
            at = theirs(s)
            tf[s] = part[2, at, :] + rpf[at, :]
            y_far[s].start()

    def far_x(i):
        for s in sub_of(i):
            y_far[s].wait_recv()
            at = mine(s)
            xs[s] = part[2, at, :] + rpf[at, :] + ryf[s]
            x_ret[s].start()

    def arrive(i):
        x_hid[i].wait_recv()
        f_hid[i].start()
        normalize(2, i * ROWS, ROWS)

    def far(i):
        f_hid[i].wait_recv()
        normalize(3, i * ROWS, ROWS)
        unit(2, i)
        c_far[i].start()

    def near(i):
        p_hid[i].wait_recv()
        normalize(1, i * ROWS, ROWS)
        unit(0, i)
        c_near[i].start()

    def shared_expert():
        for c in sh_cp:
            c.wait()
        sg = dotf(xall[0], wsg[...])
        su = dotf(xall[0], wsu[...])
        sa = (sg * jax.nn.sigmoid(sg) * su).astype(BF)
        for j in range(d_model // 256):
            cs = slice(j * 256, (j + 1) * 256)
            dense[:, cs] = dotf(sa, wsd[:, cs])

    swap = one_hot_mat(2 * kd, 2 * kd, lambda r, c: ((r // kd) == ((c // hd) % 2)) & ((r % kd) // hd == c // (2 * hd)) & (r % hd == c % hd))

    def own_y(s):
        if s % per_chunk == 0:
            c_near[s // per_chunk].wait_recv()
        at = pl.ds(s * SUB, SUB)
        ctx_bf = dotf(ctx[at, :].astype(BF), swap).astype(BF)
        for j in range(d_model // 256):
            cs = slice(j * 256, (j + 1) * 256)
            dense[at, cs] = dense[at, cs] + dotf(ctx_bf, wo[:, cs]) + part[0, at, cs] + rph[at, cs]
        ty[s] = dense[theirs(s), :]
        y_own[s].start()

    def finish(s):
        y_own[s].wait_recv()
        x_ret[s].wait_recv()
        at = mine(s)
        outb[at, :] = (hall[0, at, :].astype(F32) + (dense[at, :] + ryo[s] + rxf[s])).astype(BF)
        y_out[s].start()

    normalize(0, 0, n_rows)
    for c in qkv_cp:
        c.wait()

    nq = wq.shape[1]
    q_bf = [dotf(xall[0], wq[:, j * 256:(j + 1) * 256]).astype(BF) for j in range(nq // 256)]
    for g, ref in enumerate((q0, q1)):
        acc = None
        for j in range(nq // 256):
            def sel(r, c, j=j, g=g):
                r2 = r + j * 256
                return ((r2 // (2 * hd)) == (c // hd)) & ((r2 % (2 * hd)) == g * hd + c % hd)
            term = dotf(q_bf[j], one_hot_mat(256, kd, sel))
            acc = term if acc is None else acc + term
        ref[...] = acc
    kn[...] = dotf(xall[0], wk[...]).astype(BF).astype(F32)
    vn[...] = dotf(xall[0], wv[...]).astype(BF).astype(F32)

    for c in p_idg:
        c.wait_recv()
    gate_table(0)
    gate_table(1)
    for c in exp_cp:
        c.wait()
    near(0)
    attend(4)
    for c in x_idg:
        c.wait_recv()
    for c in f_idg:
        c.start()
    arrive(0)
    gate_table(2)
    attend(6)
    for c in f_idg:
        c.wait_recv()
    gate_table(3)
    far(0)
    attend(8)
    far_y(0)
    near(1)
    arrive(1)
    attend(10)
    far(1)
    shared_expert()
    attend(12)
    far_y(1)
    own_y(0)
    attend(14)
    far_x(0)
    attend(18)
    own_y(1)
    attend(20)
    far_x(1)
    attend(26)
    own_y(2)
    finish(0)
    attend(28)
    finish(1)
    attend(n_blk)
    own_y(3)
    finish(2)
    finish(3)
    out_cp = []
    for s in subs:
        y_out[s].wait_recv()
        at = pl.ds(s * SUB, SUB)
        c = local(outb.at[at], out_hbm.at[at], osem.at[s])
        c.start()
        out_cp.append(c)
    for c in x_hid + p_hid + f_hid + x_idg + p_idg + f_idg + c_far + c_near + y_far + x_ret + y_own + y_out:
        c.wait_send()
    for c in out_cp:
        c.wait()


def solution(mesh):
    tp_size = mesh.shape['tp']
    ep_size = mesh.shape['ep']
    tok_spec = P(('rep', 'ep'), None)
    col_spec = P(None, 'tp')
    row_spec = P('tp', None)
    cache_spec = P(('rep', 'ep'), None, 'tp', None)
    expert_spec = P(('ep', 'tp'), None, None)

    def device_step(hidden, g_norm, w_q, w_k, w_v, w_o, k_cache, v_cache, lengths, w_sh_gate, w_sh_up, w_sh_down, w_gate, w_up, w_down, expert_ids, gate_vals):
        n_rows, d = hidden.shape
        _, seq, kvh, hd = k_cache.shape
        n_local, _, ff = w_gate.shape
        fs = w_sh_gate.shape[1]
        kd = kvh * hd
        top = expert_ids.shape[1]
        k_t = k_cache.transpose(0, 2, 3, 1).reshape(n_rows, kd, seq)
        v_t = v_cache.transpose(0, 2, 3, 1).reshape(n_rows, kd, seq)
        cfg = (n_rows, kvh, hd, seq, n_local, tp_size, ep_size)
        half = SUB // tp_size
        n_chunk = n_rows // ROWS
        n_sub = n_rows // SUB
        n_remote = 5 * n_chunk + 6 + 4 * n_sub
        R = TB * 2 * kvh
        args = (hidden, g_norm.reshape(1, d), w_q, w_k, w_v, w_o, k_t, v_t, lengths, w_sh_gate, w_sh_up, w_sh_down,
                w_gate, w_up, w_down, expert_ids.T, gate_vals.T)
        v = pltpu.VMEM
        dma = pltpu.SemaphoreType.DMA
        scratch = [
            v((4, n_rows, d), BF), v((4, n_rows, d), BF), v((1, d), F32), v(w_q.shape, BF), v(w_k.shape, BF), v(w_v.shape, BF), v(w_o.shape, BF),
            v(w_sh_gate.shape, BF), v(w_sh_up.shape, BF), v(w_sh_down.shape, BF), v(w_gate.shape, BF), v(w_up.shape, BF), v(w_down.shape, BF),
            v((4, top, n_rows), jnp.int32), v((4, top, n_rows), F32), v((4, n_local, n_rows, LANES), F32),
            v((SLOTS, TB, kd, seq), BF), v((SLOTS, TB, kd, seq), BF), pltpu.SMEM((n_rows,), jnp.int32),
            v((n_rows, kd), F32), v((n_rows, kd), F32), v((n_rows, kd), F32), v((n_rows, kd), F32), v((n_rows, 2 * kd), F32),
            v((n_rows, d), F32), v((4, n_rows, d), F32), v((n_rows, d), F32), v((n_rows, d), F32), v((2 * ROWS, ff), BF), v((n_rows, d), BF),
            v((2, R, kd), F32), v((2, R, LANES), F32), v((2, R, seq), F32), v((2, R, seq), F32), v((2, R, LANES), F32),
            *[v((n_sub, half, d), F32)] * 6,
            dma((12,)), dma((3,)), dma((SLOTS,)), dma((SLOTS,)), dma((n_sub,)), dma((n_remote,)), dma((n_remote,)),
        ]
        return pl.pallas_call(
            functools.partial(layer_kernel, cfg),
            out_shape=jax.ShapeDtypeStruct((n_rows, d), BF),
            in_specs=[pl.BlockSpec(memory_space=pl.ANY)] * len(args),
            out_specs=pl.BlockSpec(memory_space=pl.ANY),
            scratch_shapes=scratch,
            compiler_params=pltpu.CompilerParams(collective_id=0, has_side_effects=True, vmem_limit_bytes=67043328),
            name='layer',
        )(*args)

    return jax.shard_map(device_step, mesh=mesh, in_specs=(tok_spec, P(None), col_spec, col_spec, col_spec, row_spec, cache_spec, cache_spec, P(('rep', 'ep')), col_spec, col_spec, row_spec, expert_spec, expert_spec, expert_spec, tok_spec, tok_spec), out_specs=tok_spec, check_vma=False)
```

```python
import functools

import jax
import jax.numpy as jnp
from jax import lax
from jax.experimental import pallas as pl
from jax.experimental.pallas import tpu as pltpu
from jax.sharding import PartitionSpec as P

RMS_EPS = 1e-6
TB = 8
EARLY = 6
SLOTS = 8
ROWS = 128
SUBS = ((0, 64), (64, 64), (128, 64), (192, 32), (224, 32))
LANES = 128
BF = jnp.bfloat16
F32 = jnp.float32


def one_hot_mat(rows, cols, fn):
    r = lax.broadcasted_iota(jnp.int32, (rows, cols), 0)
    c = lax.broadcasted_iota(jnp.int32, (rows, cols), 1)
    return jnp.where(fn(r, c), 1.0, 0.0).astype(BF)


def dotf(a, b):
    return jnp.dot(a, b, preferred_element_type=F32)


def dot_nt(a, b):
    return lax.dot_general(a, b, (((1,), (1,)), ((), ())), preferred_element_type=F32)


def layer_kernel(cfg, hid_hbm, gn_hbm, wq_hbm, wk_hbm, wv_hbm, wo_hbm, k_hbm, v_hbm, len_hbm, wsg_hbm, wsu_hbm, wsd_hbm,
                 wg_hbm, wu_hbm, wd_hbm, ids_hbm, gts_hbm, out_hbm,
                 hall, xall, gn, wq, wk, wv, wo, wsg, wsu, wsd, wg, wu, wd, idg, gtg, gb, kbuf, vbuf, lens,
                 q0, q1, kn, vn, om, dense, part, rpf, rph, act, outb, ss, sc, ps, sp, tf, ryf, xs, rxf, ty, ryo,
                 lsem, wsem, ksem, vsem, osem, s_send, s_recv):
    n_rows, kvh, hd, seq, n_local, tp_size, ep_size = cfg
    d_model = hall.shape[2]
    n_chunk = n_rows // ROWS
    n_blk = n_rows // TB
    kd = kvh * hd
    tp = lax.axis_index('tp')
    ep = lax.axis_index('ep')
    partner = {'ep': ep + 1 - 2 * lax.rem(ep, 2)}
    xnbr = {'ep': lax.rem(ep + ep_size // 2, ep_size)}
    ynbr = {'tp': 1 - tp}

    def local(src, dst, sem):
        return pltpu.make_async_copy(src, dst, sem)

    n_remote = [0]

    def remote(src, dst, dev):
        i = n_remote[0]
        n_remote[0] += 1
        return pltpu.make_async_remote_copy(src_ref=src, dst_ref=dst, send_sem=s_send.at[i], recv_sem=s_recv.at[i],
                                            device_id=dev, device_id_type=pl.DeviceIdType.MESH)

    def rows(i):
        return pl.ds(i * ROWS, ROWS)

    def mine(s):
        r0, n = SUBS[s]
        return pl.ds(pl.multiple_of(r0 + tp * (n // 2), n // 2), n // 2)

    def theirs(s):
        r0, n = SUBS[s]
        return pl.ds(pl.multiple_of(r0 + (1 - tp) * (n // 2), n // 2), n // 2)

    def packed(s):
        r0, n = SUBS[s]
        return pl.ds(r0 // 2, n // 2)

    hid_cp = [local(hid_hbm, hall.at[0], lsem.at[0])]
    small_cp = [local(ids_hbm, idg.at[0], lsem.at[1]), local(gts_hbm, gtg.at[0], lsem.at[2]),
                local(gn_hbm, gn, lsem.at[3]), local(len_hbm, lens, lsem.at[4])]
    qkv_cp = [local(wq_hbm, wq, lsem.at[5]), local(wk_hbm, wk, lsem.at[6]), local(wv_hbm, wv, lsem.at[7])]
    sh_cp = [local(wsg_hbm, wsg, lsem.at[8]), local(wsu_hbm, wsu, lsem.at[9]), local(wsd_hbm, wsd, lsem.at[10]),
             local(wo_hbm, wo, lsem.at[11])]
    exp_cp = [local(wg_hbm, wg, wsem.at[0]), local(wu_hbm, wu, wsem.at[1]), local(wd_hbm, wd, wsem.at[2])]

    def k_cp(b):
        slot = lax.rem(b, SLOTS)
        return local(k_hbm.at[pl.ds(b * TB, TB)], kbuf.at[slot], ksem.at[slot])

    def v_cp(b):
        slot = lax.rem(b, SLOTS)
        return local(v_hbm.at[pl.ds(b * TB, TB)], vbuf.at[slot], vsem.at[slot])

    for c in hid_cp + small_cp + qkv_cp:
        c.start()
    for b in range(EARLY):
        k_cp(b).start()
        v_cp(b).start()
    for c in exp_cp:
        c.start()
    for b in range(EARLY, SLOTS):
        k_cp(b).start()
        v_cp(b).start()
    for c in sh_cp:
        c.start()

    barrier = pltpu.get_barrier_semaphore()
    for dev in (partner, xnbr, ynbr):
        pl.semaphore_signal(barrier, inc=1, device_id=dev, device_id_type=pl.DeviceIdType.MESH)
    pl.semaphore_wait(barrier, 3)

    chunks = range(n_chunk)
    subs = range(len(SUBS))
    x_hid = [remote(hall.at[0, rows(i)], hall.at[2, rows(i)], xnbr) for i in chunks]
    p_hid = [remote(hall.at[0, rows(i)], hall.at[1, rows(i)], partner) for i in chunks]
    f_hid = [remote(hall.at[2, rows(i)], hall.at[3, rows(i)], partner) for i in chunks]
    x_idg = [remote(idg.at[0], idg.at[2], xnbr), remote(gtg.at[0], gtg.at[2], xnbr)]
    p_idg = [remote(idg.at[0], idg.at[1], partner), remote(gtg.at[0], gtg.at[1], partner)]
    f_idg = [remote(idg.at[2], idg.at[3], partner), remote(gtg.at[2], gtg.at[3], partner)]
    c_far = [remote(part.at[3, rows(i)], rpf.at[rows(i)], partner) for i in chunks]
    c_near = [remote(part.at[1, rows(i)], rph.at[rows(i)], partner) for i in chunks]
    y_far = [remote(tf.at[packed(s)], ryf.at[packed(s)], ynbr) for s in subs]
    x_ret = [remote(xs.at[packed(s)], rxf.at[packed(s)], xnbr) for s in subs]
    y_own = [remote(ty.at[packed(s)], ryo.at[packed(s)], ynbr) for s in subs]
    y_out = [remote(outb.at[mine(s)], outb.at[mine(s)], ynbr) for s in subs]

    for c in small_cp:
        c.wait()
    for c in x_idg + p_idg:
        c.start()
    for c in hid_cp:
        c.wait()
    for c in x_hid + p_hid:
        c.start()

    def normalize(grp, r0, n):
        def body(j, carry):
            at = pl.ds(pl.multiple_of(r0 + j * 32, 32), 32)
            h32 = hall[grp, at, :].astype(F32)
            inv = lax.rsqrt(jnp.mean(h32 * h32, axis=-1, keepdims=True) + RMS_EPS)
            xall[grp, at, :] = (h32 * inv * gn[...]).astype(BF)
            return carry
        lax.fori_loop(0, n // 32, body, 0)

    first_exp = (ep * tp_size + tp) * n_local

    def gate_table(grp):
        ids = idg[grp]
        vals = gtg[grp]
        picked = [jnp.sum(jnp.where(ids == first_exp + e, vals, 0.0), axis=0, keepdims=True) for e in range(n_local)]
        table = jnp.concatenate(picked + [jnp.zeros((LANES - n_local, n_rows), F32)], axis=0)
        cols = jnp.transpose(table)
        for e in range(n_local):
            gb[grp, e] = jnp.broadcast_to(cols[:, e:e + 1], (n_rows, LANES))

    per_tok = 2 * kvh
    R = TB * per_tok
    rr = lax.broadcasted_iota(jnp.int32, (per_tok, kd), 0)
    cc = lax.broadcasted_iota(jnp.int32, (per_tok, kd), 1)
    own = (rr % kvh) == (cc // hd)
    low = rr < kvh
    pos = lax.broadcasted_iota(jnp.int32, (per_tok, seq), 1)
    scale = hd ** -0.5

    def heads(t):
        return slice(t * per_tok, (t + 1) * per_tok)

    def spread(ref, tok):
        return jnp.broadcast_to(ref[pl.ds(tok, 1), :], (per_tok, kd))

    def stage_kv(b, p, with_v=True, with_k=True):
        for t in range(TB):
            if with_k:
                tok = b * TB + t
                q_t = jnp.where(own, jnp.where(low, spread(q0, tok), spread(q1, tok)), 0.0)
                s_t = dotf(q_t.astype(BF), kbuf[lax.rem(b, SLOTS), t])
                sc[p, heads(t), :] = jnp.where(pos < lens[tok], s_t * scale, -1e30)
                self_t = jnp.sum(q_t * spread(kn, tok), axis=-1, keepdims=True) * scale
                ss[p, heads(t), :] = jnp.broadcast_to(self_t, (per_tok, LANES))
            if with_v:
                tok = (b - 2) * TB + t
                o_t = dot_nt(ps[p, heads(t), :].astype(BF), vbuf[lax.rem(b - 2, SLOTS), t])
                o_t = o_t + jnp.concatenate([sp[p, heads(t), :]] * (kd // LANES), axis=1) * spread(vn, tok)
                om[pl.ds(pl.multiple_of(tok * per_tok, per_tok), per_tok), :] = jnp.where(own, o_t, 0.0)

    def stage_s(p):
        scores = sc[p]
        self_score = ss[p, :, 0:1]
        peak = jnp.maximum(jnp.max(scores, axis=-1, keepdims=True), self_score)
        prob = jnp.exp(scores - peak)
        self_prob = jnp.exp(self_score - peak)
        inv = 1.0 / (jnp.sum(prob, axis=-1, keepdims=True) + self_prob)
        ps[p] = prob * inv
        sp[p] = jnp.broadcast_to((self_prob * inv).astype(BF).astype(F32), (R, LANES))

    def attn_pair(j, carry):
        b = 2 * j
        for p in range(2):
            k_cp(b + p).wait()
            v_cp(b + p - 2).wait()
        for p in range(2):
            stage_kv(b + p, p)
            stage_s(1 - p)
        for p in range(2):
            @pl.when(b + p + SLOTS < n_blk)
            def _():
                k_cp(b + p + SLOTS).start()

            @pl.when(b + p - 2 + SLOTS < n_blk)
            def _():
                v_cp(b + p - 2 + SLOTS).start()
        return carry

    done = [0]

    def attend(hi):
        lo = done[0]
        done[0] = hi
        if lo == 0:
            for p in range(2):
                k_cp(p).wait()
            for p in range(2):
                stage_kv(p, p, with_v=False)
            stage_s(0)
            for p in range(2):
                k_cp(p + SLOTS).start()
            lo = 2
        lax.fori_loop(lo // 2, hi // 2, attn_pair, 0)
        if hi == n_blk:
            for p in range(2):
                v_cp(n_blk - 2 + p).wait()
            stage_kv(n_blk, 0, with_k=False)
            stage_s(1)
            stage_kv(n_blk + 1, 1, with_k=False)

    ff = wg.shape[2]

    def unit(g0, r0, n):
        at = pl.ds(r0, n)
        m2 = 2 * n

        xr = xall[g0:g0 + 2, at, :].reshape(m2, d_model)

        def up(e, j):
            cs = slice(j * 256, (j + 1) * 256)
            g_a = dotf(xr, wg[e, :, cs])
            u_b = dotf(xr, wu[e, :, cs])
            act[e % 2, :, cs] = (g_a * jax.nn.sigmoid(g_a) * u_b).astype(BF)

        def down(e, j):
            gate = gb[g0:g0 + 2, e, at, :].reshape(m2, LANES)
            y = dotf(act[e % 2], wd[e, :, j * 256:(j + 1) * 256]).astype(BF).astype(F32)
            for m in range(256 // LANES):
                ls = slice(j * 256 + m * LANES, j * 256 + (m + 1) * LANES)
                add = jnp.where(gate > 0.0, gate * y[:, m * LANES:(m + 1) * LANES], 0.0).reshape(2, n, LANES)
                part[g0:g0 + 2, at, ls] = add if e == 0 else part[g0:g0 + 2, at, ls] + add

        n_up = ff // 256
        n_down = d_model // 256
        for e in range(n_local + 1):
            for j in range(n_up):
                if e < n_local:
                    up(e, j)
                if e > 0:
                    for k in range(j * n_down // n_up, (j + 1) * n_down // n_up):
                        down(e - 1, k)

    def sub_of(i):
        return [s for s in subs if SUBS[s][0] // ROWS == i]

    def far_y(i):
        c_far[i].wait_recv()
        for s in sub_of(i):
            at = theirs(s)
            tf[packed(s), :] = part[2, at, :] + rpf[at, :]
            y_far[s].start()

    def far_x(i):
        for s in sub_of(i):
            y_far[s].wait_recv()
            at = mine(s)
            xs[packed(s), :] = part[2, at, :] + rpf[at, :] + ryf[packed(s), :]
            x_ret[s].start()

    def arrive(i):
        x_hid[i].wait_recv()
        f_hid[i].start()
        normalize(2, i * ROWS, ROWS)

    def far(i):
        f_hid[i].wait_recv()
        normalize(3, i * ROWS, ROWS)
        unit(2, i * ROWS, ROWS)
        c_far[i].start()

    def near(i):
        p_hid[i].wait_recv()
        normalize(1, i * ROWS, ROWS)
        unit(0, i * ROWS, ROWS)
        c_near[i].start()

    def shared_expert():
        for c in sh_cp:
            c.wait()
        sg = dotf(xall[0], wsg[...])
        su = dotf(xall[0], wsu[...])
        sa = (sg * jax.nn.sigmoid(sg) * su).astype(BF)
        for j in range(d_model // 256):
            cs = slice(j * 256, (j + 1) * 256)
            dense[:, cs] = dotf(sa, wsd[:, cs])

    swap = one_hot_mat(2 * kd, 2 * kd, lambda r, c: ((r // kd) == ((c // hd) % 2)) & ((r % kd) // hd == c // (2 * hd)) & (r % hd == c % hd))

    def own_y(s):
        r0, n = SUBS[s]
        if s in (sub_of(0)[0], sub_of(1)[0]):
            c_near[r0 // ROWS].wait_recv()
        at = pl.ds(r0, n)
        gather_o = one_hot_mat(2 * n, n * per_tok, lambda r, c: (c // per_tok == r % n) & ((c % per_tok) // kvh == r // n))
        o2 = dotf(gather_o, om[pl.ds(r0 * per_tok, n * per_tok), :].astype(BF)).astype(BF)
        ctx_bf = dotf(jnp.concatenate([o2[0:n], o2[n:2 * n]], axis=1), swap).astype(BF)
        for j in range(d_model // 256):
            cs = slice(j * 256, (j + 1) * 256)
            dense[at, cs] = dense[at, cs] + dotf(ctx_bf, wo[:, cs]) + part[0, at, cs] + rph[at, cs]
        ty[packed(s), :] = dense[theirs(s), :]
        y_own[s].start()

    def finish(s):
        y_own[s].wait_recv()
        x_ret[s].wait_recv()
        at = mine(s)
        outb[at, :] = (hall[0, at, :].astype(F32) + (dense[at, :] + ryo[packed(s), :] + rxf[packed(s), :])).astype(BF)
        y_out[s].start()

    normalize(0, 0, n_rows)
    for c in qkv_cp:
        c.wait()

    nq = wq.shape[1]
    q_bf = [dotf(xall[0], wq[:, j * 256:(j + 1) * 256]).astype(BF) for j in range(nq // 256)]
    for g, ref in enumerate((q0, q1)):
        acc = None
        for j in range(nq // 256):
            def sel(r, c, j=j, g=g):
                r2 = r + j * 256
                return ((r2 // (2 * hd)) == (c // hd)) & ((r2 % (2 * hd)) == g * hd + c % hd)
            term = dotf(q_bf[j], one_hot_mat(256, kd, sel))
            acc = term if acc is None else acc + term
        ref[...] = acc
    kn[...] = dotf(xall[0], wk[...]).astype(BF).astype(F32)
    vn[...] = dotf(xall[0], wv[...]).astype(BF).astype(F32)

    attend(8)
    for c in p_idg + x_idg:
        c.wait_recv()
    for c in f_idg:
        c.start()
    gate_table(0)
    gate_table(1)
    gate_table(2)
    attend(10)
    arrive(0)
    for c in exp_cp:
        c.wait()
    attend(12)
    for c in f_idg:
        c.wait_recv()
    gate_table(3)
    far(0)
    arrive(1)
    attend(14)
    far_y(0)
    far(1)
    attend(18)
    far_y(1)
    near(0)
    shared_expert()
    far_x(0)
    near(1)
    own_y(0)
    own_y(1)
    attend(22)
    far_x(1)
    attend(26)
    own_y(2)
    finish(0)
    finish(1)
    attend(30)
    own_y(3)
    finish(2)
    attend(n_blk)
    own_y(4)
    finish(3)
    finish(4)
    out_cp = []
    for s in subs:
        y_out[s].wait_recv()
        at = pl.ds(*SUBS[s])
        c = local(outb.at[at], out_hbm.at[at], osem.at[s])
        c.start()
        out_cp.append(c)
    for c in x_hid + p_hid + f_hid + x_idg + p_idg + f_idg + c_far + c_near + y_far + x_ret + y_own + y_out:
        c.wait_send()
    for c in out_cp:
        c.wait()


def solution(mesh):
    tp_size = mesh.shape['tp']
    ep_size = mesh.shape['ep']
    tok_spec = P(('rep', 'ep'), None)
    col_spec = P(None, 'tp')
    row_spec = P('tp', None)
    cache_spec = P(('rep', 'ep'), None, 'tp', None)
    expert_spec = P(('ep', 'tp'), None, None)

    def device_step(hidden, g_norm, w_q, w_k, w_v, w_o, k_cache, v_cache, lengths, w_sh_gate, w_sh_up, w_sh_down, w_gate, w_up, w_down, expert_ids, gate_vals):
        n_rows, d = hidden.shape
        _, seq, kvh, hd = k_cache.shape
        n_local, _, ff = w_gate.shape
        fs = w_sh_gate.shape[1]
        kd = kvh * hd
        top = expert_ids.shape[1]
        k_t = k_cache.transpose(0, 2, 3, 1).reshape(n_rows, kd, seq)
        v_t = v_cache.transpose(0, 2, 3, 1).reshape(n_rows, kd, seq)
        cfg = (n_rows, kvh, hd, seq, n_local, tp_size, ep_size)
        n_chunk = n_rows // ROWS
        n_sub = len(SUBS)
        n_remote = 5 * n_chunk + 6 + 4 * n_sub
        R = TB * 2 * kvh
        args = (hidden, g_norm.reshape(1, d), w_q, w_k, w_v, w_o, k_t, v_t, lengths, w_sh_gate, w_sh_up, w_sh_down,
                w_gate, w_up, w_down, expert_ids.T, gate_vals.T)
        v = pltpu.VMEM
        dma = pltpu.SemaphoreType.DMA
        scratch = [
            v((4, n_rows, d), BF), v((4, n_rows, d), BF), v((1, d), F32), v(w_q.shape, BF), v(w_k.shape, BF), v(w_v.shape, BF), v(w_o.shape, BF),
            v(w_sh_gate.shape, BF), v(w_sh_up.shape, BF), v(w_sh_down.shape, BF), v(w_gate.shape, BF), v(w_up.shape, BF), v(w_down.shape, BF),
            v((4, top, n_rows), jnp.int32), v((4, top, n_rows), F32), v((4, n_local, n_rows, LANES), F32),
            v((SLOTS, TB, kd, seq), BF), v((SLOTS, TB, kd, seq), BF), pltpu.SMEM((n_rows,), jnp.int32),
            v((n_rows, kd), F32), v((n_rows, kd), F32), v((n_rows, kd), F32), v((n_rows, kd), F32), v((n_rows * 2 * kvh, kd), F32),
            v((n_rows, d), F32), v((4, n_rows, d), F32), v((n_rows, d), F32), v((n_rows, d), F32), v((2, 2 * ROWS, ff), BF), v((n_rows, d), BF),
            v((2, R, LANES), F32), v((2, R, seq), F32), v((2, R, seq), F32), v((2, R, LANES), F32),
            *[v((n_rows // 2, d), F32)] * 6,
            dma((12,)), dma((3,)), dma((SLOTS,)), dma((SLOTS,)), dma((n_sub,)), dma((n_remote,)), dma((n_remote,)),
        ]
        return pl.pallas_call(
            functools.partial(layer_kernel, cfg),
            out_shape=jax.ShapeDtypeStruct((n_rows, d), BF),
            in_specs=[pl.BlockSpec(memory_space=pl.ANY)] * len(args),
            out_specs=pl.BlockSpec(memory_space=pl.ANY),
            scratch_shapes=scratch,
            compiler_params=pltpu.CompilerParams(collective_id=0, has_side_effects=True, vmem_limit_bytes=67043328),
            name='layer',
        )(*args)

    return jax.shard_map(device_step, mesh=mesh, in_specs=(tok_spec, P(None), col_spec, col_spec, col_spec, row_spec, cache_spec, cache_spec, P(('rep', 'ep')), col_spec, col_spec, row_spec, expert_spec, expert_spec, expert_spec, tok_spec, tok_spec), out_specs=tok_spec, check_vma=False)
```

```python
import functools

import jax
import jax.numpy as jnp
from jax import lax
from jax.experimental import pallas as pl
from jax.experimental.pallas import tpu as pltpu
from jax.sharding import PartitionSpec as P

RMS_EPS = 1e-6
TB = 8
EARLY = 6
SLOTS = 8
ROWS = 128
SUBS = ((0, 64), (64, 64), (128, 64), (192, 32), (224, 32))
LANES = 128
BF = jnp.bfloat16
F32 = jnp.float32


def one_hot_mat(rows, cols, fn):
    r = lax.broadcasted_iota(jnp.int32, (rows, cols), 0)
    c = lax.broadcasted_iota(jnp.int32, (rows, cols), 1)
    return jnp.where(fn(r, c), 1.0, 0.0).astype(BF)


def dotf(a, b):
    return jnp.dot(a, b, preferred_element_type=F32)


def dot_nt(a, b):
    return lax.dot_general(a, b, (((1,), (1,)), ((), ())), preferred_element_type=F32)


def layer_kernel(cfg, hid_hbm, gn_hbm, wq_hbm, wk_hbm, wv_hbm, wo_hbm, k_hbm, v_hbm, len_hbm, wsg_hbm, wsu_hbm, wsd_hbm,
                 wg_hbm, wu_hbm, wd_hbm, ids_hbm, gts_hbm, out_hbm,
                 hall, xall, gn, wq, wk, wv, wo, wsg, wsu, wsd, wg, wu, wd, idg, gtg, gb, kbuf, vbuf, lens,
                 q0, q1, kn, vn, om, dense, part, rpf, rph, act, outb, ss, sc, ps, sp, tf, ryf, xs, rxf, ty, ryo, xa, rxa, ryl,
                 lsem, wsem, ksem, vsem, osem, s_send, s_recv):
    n_rows, kvh, hd, seq, n_local, tp_size, ep_size = cfg
    d_model = hall.shape[2]
    n_chunk = n_rows // ROWS
    n_blk = n_rows // TB
    kd = kvh * hd
    tp = lax.axis_index('tp')
    ep = lax.axis_index('ep')
    partner = {'ep': ep + 1 - 2 * lax.rem(ep, 2)}
    xnbr = {'ep': lax.rem(ep + ep_size // 2, ep_size)}
    ynbr = {'tp': 1 - tp}

    def local(src, dst, sem):
        return pltpu.make_async_copy(src, dst, sem)

    n_remote = [0]

    def remote(src, dst, dev):
        i = n_remote[0]
        n_remote[0] += 1
        return pltpu.make_async_remote_copy(src_ref=src, dst_ref=dst, send_sem=s_send.at[i], recv_sem=s_recv.at[i],
                                            device_id=dev, device_id_type=pl.DeviceIdType.MESH)

    def rows(i):
        return pl.ds(i * ROWS, ROWS)

    def mine(s):
        r0, n = SUBS[s]
        return pl.ds(pl.multiple_of(r0 + tp * (n // 2), n // 2), n // 2)

    def theirs(s):
        r0, n = SUBS[s]
        return pl.ds(pl.multiple_of(r0 + (1 - tp) * (n // 2), n // 2), n // 2)

    def packed(s):
        r0, n = SUBS[s]
        return pl.ds(r0 // 2, n // 2)

    hid_cp = [local(hid_hbm, hall.at[0], lsem.at[0])]
    small_cp = [local(ids_hbm, idg.at[0], lsem.at[1]), local(gts_hbm, gtg.at[0], lsem.at[2]),
                local(gn_hbm, gn, lsem.at[3]), local(len_hbm, lens, lsem.at[4])]
    qkv_cp = [local(wq_hbm, wq, lsem.at[5]), local(wk_hbm, wk, lsem.at[6]), local(wv_hbm, wv, lsem.at[7])]
    sh_cp = [local(wsg_hbm, wsg, lsem.at[8]), local(wsu_hbm, wsu, lsem.at[9]), local(wsd_hbm, wsd, lsem.at[10]),
             *[local(wo_hbm.at[pl.ds((h * 2 + g) * hd, hd)], wo.at[pl.ds((g * kvh + h) * hd, hd)], osem.at[len(SUBS) + g * kvh + h])
               for g in range(2) for h in range(kvh)]]
    exp_cp = [local(wg_hbm, wg, wsem.at[0]), local(wu_hbm, wu, wsem.at[1]), local(wd_hbm, wd, wsem.at[2])]

    def k_cp(b):
        slot = lax.rem(b, SLOTS)
        return local(k_hbm.at[pl.ds(b * TB, TB)], kbuf.at[slot], ksem.at[slot])

    def v_cp(b):
        slot = lax.rem(b, SLOTS)
        return local(v_hbm.at[pl.ds(b * TB, TB)], vbuf.at[slot], vsem.at[slot])

    for c in hid_cp + small_cp + qkv_cp:
        c.start()
    for b in range(EARLY):
        k_cp(b).start()
        v_cp(b).start()
    for c in exp_cp:
        c.start()
    for b in range(EARLY, SLOTS):
        k_cp(b).start()
        v_cp(b).start()
    for c in sh_cp:
        c.start()

    barrier = pltpu.get_barrier_semaphore()
    for dev in (partner, xnbr, ynbr):
        pl.semaphore_signal(barrier, inc=1, device_id=dev, device_id_type=pl.DeviceIdType.MESH)
    pl.semaphore_wait(barrier, 3)

    def whole(s):
        return pl.ds(*SUBS[s])

    chunks = range(n_chunk)
    subs = range(len(SUBS))

    def sub_of(i):
        return [s for s in subs if SUBS[s][0] // ROWS == i]

    x_hid = [remote(hall.at[0, rows(i)], hall.at[2, rows(i)], xnbr) for i in chunks]
    p_hid = [remote(hall.at[0, rows(i)], hall.at[1, rows(i)], partner) for i in chunks]
    f_hid = [remote(hall.at[2, rows(i)], hall.at[3, rows(i)], partner) for i in chunks]
    x_idg = [remote(idg.at[0], idg.at[2], xnbr), remote(gtg.at[0], gtg.at[2], xnbr)]
    p_idg = [remote(idg.at[0], idg.at[1], partner), remote(gtg.at[0], gtg.at[1], partner)]
    f_idg = [remote(idg.at[2], idg.at[3], partner), remote(gtg.at[2], gtg.at[3], partner)]
    c_far = [remote(part.at[3, rows(i)], rpf.at[rows(i)], partner) for i in chunks]
    c_near = [remote(part.at[1, rows(i)], rph.at[rows(i)], partner) for i in chunks]
    def packed2(s):
        return pl.ds(first.index(s) * SUBS[s][1], SUBS[s][1])

    first, last = [2], subs[-1]
    far_subs = [s for s in subs if s not in first]
    x_all = {s: remote(xa.at[packed2(s)], rxa.at[packed2(s)], xnbr) for s in first}
    y_last = remote(dense.at[whole(last)], ryl, ynbr)
    y_far = {s: remote(tf.at[packed(s)], ryf.at[packed(s)], ynbr) for s in far_subs}
    x_ret = {s: remote(xs.at[packed(s)], rxf.at[packed(s)], xnbr) for s in far_subs}
    y_own = [remote(ty.at[packed(s)], ryo.at[packed(s)], ynbr) for s in subs[:-1]]
    y_out = [remote(outb.at[mine(s)], outb.at[mine(s)], ynbr) for s in subs[:-1]]

    for c in small_cp:
        c.wait()
    for c in x_idg + p_idg:
        c.start()
    for c in hid_cp:
        c.wait()
    for c in x_hid + p_hid:
        c.start()

    def normalize(grp, r0, n):
        def body(j, carry):
            for k in range(4):
                at = pl.ds(pl.multiple_of(r0 + j * 128 + k * 32, 32), 32)
                h32 = hall[grp, at, :].astype(F32)
                inv = lax.rsqrt(jnp.mean(h32 * h32, axis=-1, keepdims=True) + RMS_EPS)
                xall[grp, at, :] = (h32 * inv * gn[...]).astype(BF)
            return carry
        lax.fori_loop(0, n // 128, body, 0)

    first_exp = (ep * tp_size + tp) * n_local

    def gate_table(grp):
        ids = idg[grp]
        vals = gtg[grp]
        picked = [jnp.sum(jnp.where(ids == first_exp + e, vals, 0.0), axis=0, keepdims=True) for e in range(n_local)]
        table = jnp.concatenate(picked + [jnp.zeros((LANES - n_local, n_rows), F32)], axis=0)
        cols = jnp.transpose(table)
        for e in range(n_local):
            gb[grp, e] = jnp.broadcast_to(cols[:, e:e + 1], (n_rows, LANES))

    per_tok = 2 * kvh
    R = TB * per_tok
    rr = lax.broadcasted_iota(jnp.int32, (per_tok, kd), 0)
    cc = lax.broadcasted_iota(jnp.int32, (per_tok, kd), 1)
    own = (rr % kvh) == (cc // hd)
    low = rr < kvh
    pos = lax.broadcasted_iota(jnp.int32, (per_tok, seq), 1)
    scale = hd ** -0.5

    def heads(t):
        return slice(t * per_tok, (t + 1) * per_tok)

    def spread(ref, tok):
        return jnp.broadcast_to(ref[pl.ds(tok, 1), :], (per_tok, kd))

    def stage_kv(b, p, with_v=True, with_k=True):
        for t in range(TB):
            if with_k:
                tok = b * TB + t
                q_t = jnp.where(own, jnp.where(low, spread(q0, tok), spread(q1, tok)), 0.0)
                s_t = dotf(q_t.astype(BF), kbuf[lax.rem(b, SLOTS), t])
                sc[p, heads(t), :] = jnp.where(pos < lens[tok], s_t * scale, -1e30)
                self_t = jnp.sum(q_t * spread(kn, tok), axis=-1, keepdims=True) * scale
                ss[p, heads(t), :] = jnp.broadcast_to(self_t, (per_tok, LANES))
            if with_v:
                tok = (b - 2) * TB + t
                o_t = dot_nt(ps[p, heads(t), :].astype(BF), vbuf[lax.rem(b - 2, SLOTS), t])
                o_t = o_t + jnp.concatenate([sp[p, heads(t), :]] * (kd // LANES), axis=1) * spread(vn, tok)
                om[pl.ds(pl.multiple_of(tok * per_tok, per_tok), per_tok), :] = jnp.where(own, o_t, 0.0)

    def stage_s(p):
        scores = sc[p]
        self_score = ss[p, :, 0:1]
        peak = jnp.maximum(jnp.max(scores, axis=-1, keepdims=True), self_score)
        prob = jnp.exp(scores - peak)
        self_prob = jnp.exp(self_score - peak)
        inv = 1.0 / (jnp.sum(prob, axis=-1, keepdims=True) + self_prob)
        ps[p] = prob * inv
        sp[p] = jnp.broadcast_to((self_prob * inv).astype(BF).astype(F32), (R, LANES))

    def attn_pair(j, carry):
        b = 2 * j
        for p in range(2):
            k_cp(b + p).wait()
            v_cp(b + p - 2).wait()
        for p in range(2):
            stage_kv(b + p, p)
            stage_s(1 - p)
        for p in range(2):
            @pl.when(b + p + SLOTS < n_blk)
            def _():
                k_cp(b + p + SLOTS).start()

            @pl.when(b + p - 2 + SLOTS < n_blk)
            def _():
                v_cp(b + p - 2 + SLOTS).start()
        return carry

    done = [0]

    def attend(hi):
        lo = done[0]
        done[0] = hi
        if lo == 0:
            for p in range(2):
                k_cp(p).wait()
            for p in range(2):
                stage_kv(p, p, with_v=False)
            stage_s(0)
            for p in range(2):
                k_cp(p + SLOTS).start()
            lo = 2
        lax.fori_loop(lo // 2, hi // 2, attn_pair, 0)
        if hi == n_blk:
            for p in range(2):
                v_cp(n_blk - 2 + p).wait()
            stage_kv(n_blk, 0, with_k=False)
            stage_s(1)
            stage_kv(n_blk + 1, 1, with_k=False)

    ff = wg.shape[2]

    def unit(g0, r0, n):
        at = pl.ds(r0, n)
        m2 = 2 * n

        xr = xall[g0:g0 + 2, at, :].reshape(m2, d_model)

        def up(e, j):
            cs = slice(j * 256, (j + 1) * 256)
            g_a = dotf(xr, wg[e, :, cs])
            u_b = dotf(xr, wu[e, :, cs])
            act[e % 2, :, cs] = (g_a * jax.nn.sigmoid(g_a) * u_b).astype(BF)

        def down(e, j):
            gate = gb[g0:g0 + 2, e, at, :].reshape(m2, LANES)
            y = dotf(act[e % 2], wd[e, :, j * 256:(j + 1) * 256]).astype(BF).astype(F32)
            for m in range(256 // LANES):
                ls = slice(j * 256 + m * LANES, j * 256 + (m + 1) * LANES)
                add = jnp.where(gate > 0.0, gate * y[:, m * LANES:(m + 1) * LANES], 0.0).reshape(2, n, LANES)
                part[g0:g0 + 2, at, ls] = add if e == 0 else part[g0:g0 + 2, at, ls] + add

        n_up = ff // 256
        n_down = d_model // 256
        for e in range(n_local + 1):
            for j in range(n_up):
                if e < n_local:
                    up(e, j)
                if e > 0:
                    for k in range(j * n_down // n_up, (j + 1) * n_down // n_up):
                        down(e - 1, k)

    def far_send(i):
        c_far[i].wait_recv()
        for s in sub_of(i)[::-1]:
            if s in first:
                at = whole(s)
                xa[packed2(s), :] = part[2, at, :] + rpf[at, :]
                x_all[s].start()
            else:
                at = theirs(s)
                tf[packed(s), :] = part[2, at, :] + rpf[at, :]
                y_far[s].start()

    def far_x(some):
        for s in some:
            y_far[s].wait_recv()
            at = mine(s)
            xs[packed(s), :] = part[2, at, :] + rpf[at, :] + ryf[packed(s), :]
            x_ret[s].start()

    def arrive(i):
        x_hid[i].wait_recv()
        f_hid[i].start()
        normalize(2, i * ROWS, ROWS)

    def far(i):
        f_hid[i].wait_recv()
        normalize(3, i * ROWS, ROWS)
        unit(2, i * ROWS, ROWS)
        c_far[i].start()

    def near(i):
        p_hid[i].wait_recv()
        normalize(1, i * ROWS, ROWS)
        unit(0, i * ROWS, ROWS)
        c_near[i].start()

    def shared_expert():
        for c in sh_cp:
            c.wait()
        sg = dotf(xall[0], wsg[...])
        su = dotf(xall[0], wsu[...])
        sa = (sg * jax.nn.sigmoid(sg) * su).astype(BF)
        for j in range(d_model // 256):
            cs = slice(j * 256, (j + 1) * 256)
            dense[:, cs] = dotf(sa, wsd[:, cs])

    def own_y(s):
        r0, n = SUBS[s]
        if s in (sub_of(0)[0], sub_of(1)[0]):
            c_near[r0 // ROWS].wait_recv()
        at = pl.ds(r0, n)
        gather_o = one_hot_mat(2 * n, n * per_tok, lambda r, c: (c // per_tok == r % n) & ((c % per_tok) // kvh == r // n))
        o2 = dotf(gather_o, om[pl.ds(r0 * per_tok, n * per_tok), :].astype(BF)).astype(BF)
        ctx_bf = jnp.concatenate([o2[0:n], o2[n:2 * n]], axis=1)
        if s in first:
            x_all[s].wait_recv()
        for j in range(d_model // 256):
            cs = slice(j * 256, (j + 1) * 256)
            total = dense[at, cs] + dotf(ctx_bf, wo[:, cs]) + part[0, at, cs] + rph[at, cs]
            dense[at, cs] = total + rxa[packed2(s), cs] if s in first else total
        if s == last:
            x_ret[s].wait_recv()
            dense[mine(s), :] = dense[mine(s), :] + rxf[packed(s), :]
            y_last.start()
        else:
            ty[packed(s), :] = dense[theirs(s), :]
            y_own[s].start()

    def finish(s):
        if s == last:
            at = whole(s)
            y_last.wait_recv()
            outb[at, :] = (hall[0, at, :].astype(F32) + (dense[at, :] + ryl[...])).astype(BF)
            return
        at = mine(s)
        y_own[s].wait_recv()
        total = dense[at, :] + ryo[packed(s), :]
        if s in far_subs:
            x_ret[s].wait_recv()
            total = total + rxf[packed(s), :]
        outb[at, :] = (hall[0, at, :].astype(F32) + total).astype(BF)
        y_out[s].start()

    normalize(0, 0, n_rows)
    for c in qkv_cp:
        c.wait()

    nq = wq.shape[1]
    q_bf = [dotf(xall[0], wq[:, j * 256:(j + 1) * 256]).astype(BF) for j in range(nq // 256)]
    for g, ref in enumerate((q0, q1)):
        acc = None
        for j in range(nq // 256):
            def sel(r, c, j=j, g=g):
                r2 = r + j * 256
                return ((r2 // (2 * hd)) == (c // hd)) & ((r2 % (2 * hd)) == g * hd + c % hd)
            term = dotf(q_bf[j], one_hot_mat(256, kd, sel))
            acc = term if acc is None else acc + term
        ref[...] = acc
    kn[...] = dotf(xall[0], wk[...]).astype(BF).astype(F32)
    vn[...] = dotf(xall[0], wv[...]).astype(BF).astype(F32)

    attend(6)
    for c in p_idg + x_idg:
        c.wait_recv()
    for c in f_idg:
        c.start()
    gate_table(0)
    gate_table(1)
    gate_table(2)
    for c in exp_cp:
        c.wait()
    near(0)
    arrive(0)
    attend(8)
    for c in f_idg:
        c.wait_recv()
    gate_table(3)
    far(0)
    arrive(1)
    attend(12)
    far_send(0)
    far(1)
    shared_expert()
    own_y(0)
    attend(14)
    far_send(1)
    near(1)
    far_x([0, 1])
    attend(18)
    own_y(1)
    attend(22)
    far_x([4, 3])
    attend(26)
    finish(0)
    own_y(2)
    attend(30)
    own_y(3)
    finish(1)
    attend(n_blk)
    own_y(4)
    finish(2)
    finish(3)
    finish(4)
    out_cp = []
    for s in subs:
        if s != last:
            y_out[s].wait_recv()
        at = whole(s)
        c = local(outb.at[at], out_hbm.at[at], osem.at[s])
        c.start()
        out_cp.append(c)
    for c in x_hid + p_hid + f_hid + x_idg + p_idg + f_idg + c_far + c_near + list(x_all.values()) + list(y_far.values()) + list(x_ret.values()) + y_own + y_out + [y_last]:
        c.wait_send()
    for c in out_cp:
        c.wait()


def solution(mesh):
    tp_size = mesh.shape['tp']
    ep_size = mesh.shape['ep']
    tok_spec = P(('rep', 'ep'), None)
    col_spec = P(None, 'tp')
    row_spec = P('tp', None)
    cache_spec = P(('rep', 'ep'), None, 'tp', None)
    expert_spec = P(('ep', 'tp'), None, None)

    def device_step(hidden, g_norm, w_q, w_k, w_v, w_o, k_cache, v_cache, lengths, w_sh_gate, w_sh_up, w_sh_down, w_gate, w_up, w_down, expert_ids, gate_vals):
        n_rows, d = hidden.shape
        _, seq, kvh, hd = k_cache.shape
        n_local, _, ff = w_gate.shape
        fs = w_sh_gate.shape[1]
        kd = kvh * hd
        top = expert_ids.shape[1]
        k_t = k_cache.transpose(0, 2, 3, 1).reshape(n_rows, kd, seq)
        v_t = v_cache.transpose(0, 2, 3, 1).reshape(n_rows, kd, seq)
        cfg = (n_rows, kvh, hd, seq, n_local, tp_size, ep_size)
        n_chunk = n_rows // ROWS
        n_sub = len(SUBS)
        n_remote = 5 * n_chunk + 6 + 4 * n_sub
        R = TB * 2 * kvh
        args = (hidden, g_norm.reshape(1, d), w_q, w_k, w_v, w_o, k_t, v_t, lengths, w_sh_gate, w_sh_up, w_sh_down,
                w_gate, w_up, w_down, expert_ids.T, gate_vals.T)
        v = pltpu.VMEM
        dma = pltpu.SemaphoreType.DMA
        scratch = [
            v((4, n_rows, d), BF), v((4, n_rows, d), BF), v((1, d), F32), v(w_q.shape, BF), v(w_k.shape, BF), v(w_v.shape, BF), v(w_o.shape, BF),
            v(w_sh_gate.shape, BF), v(w_sh_up.shape, BF), v(w_sh_down.shape, BF), v(w_gate.shape, BF), v(w_up.shape, BF), v(w_down.shape, BF),
            v((4, top, n_rows), jnp.int32), v((4, top, n_rows), F32), v((4, n_local, n_rows, LANES), F32),
            v((SLOTS, TB, kd, seq), BF), v((SLOTS, TB, kd, seq), BF), pltpu.SMEM((n_rows,), jnp.int32),
            v((n_rows, kd), F32), v((n_rows, kd), F32), v((n_rows, kd), F32), v((n_rows, kd), F32), v((n_rows * 2 * kvh, kd), F32),
            v((n_rows, d), F32), v((4, n_rows, d), F32), v((n_rows, d), F32), v((n_rows, d), F32), v((2, 2 * ROWS, ff), BF), v((n_rows, d), BF),
            v((2, R, LANES), F32), v((2, R, seq), F32), v((2, R, seq), F32), v((2, R, LANES), F32),
            *[v((n_rows // 2, d), F32)] * 6, v((ROWS, d), F32), v((ROWS, d), F32), v((SUBS[-1][1], d), F32),
            dma((12,)), dma((3,)), dma((SLOTS,)), dma((SLOTS,)), dma((n_sub + 2 * kvh,)), dma((n_remote,)), dma((n_remote,)),
        ]
        return pl.pallas_call(
            functools.partial(layer_kernel, cfg),
            out_shape=jax.ShapeDtypeStruct((n_rows, d), BF),
            in_specs=[pl.BlockSpec(memory_space=pl.ANY)] * len(args),
            out_specs=pl.BlockSpec(memory_space=pl.ANY),
            scratch_shapes=scratch,
            compiler_params=pltpu.CompilerParams(collective_id=0, has_side_effects=True, vmem_limit_bytes=67043328),
            name='layer',
        )(*args)

    return jax.shard_map(device_step, mesh=mesh, in_specs=(tok_spec, P(None), col_spec, col_spec, col_spec, row_spec, cache_spec, cache_spec, P(('rep', 'ep')), col_spec, col_spec, row_spec, expert_spec, expert_spec, expert_spec, tok_spec, tok_spec), out_specs=tok_spec, check_vma=False)
```

```python
import functools

import jax
import jax.numpy as jnp
from jax import lax
from jax.experimental import pallas as pl
from jax.experimental.pallas import tpu as pltpu
from jax.sharding import PartitionSpec as P

RMS_EPS = 1e-6
TB = 8
EARLY = 6
SLOTS = 8
ROWS = 128
SUBS = ((0, 64), (64, 64), (128, 64), (192, 32), (224, 16), (240, 16))
LANES = 128
BF = jnp.bfloat16
F32 = jnp.float32


def one_hot_mat(rows, cols, fn):
    r = lax.broadcasted_iota(jnp.int32, (rows, cols), 0)
    c = lax.broadcasted_iota(jnp.int32, (rows, cols), 1)
    return jnp.where(fn(r, c), 1.0, 0.0).astype(BF)


def dotf(a, b):
    return jnp.dot(a, b, preferred_element_type=F32)


def dot_nt(a, b):
    return lax.dot_general(a, b, (((1,), (1,)), ((), ())), preferred_element_type=F32)


def layer_kernel(cfg, hid_hbm, gn_hbm, wq_hbm, wk_hbm, wv_hbm, wo_hbm, k_hbm, v_hbm, len_hbm, wsg_hbm, wsu_hbm, wsd_hbm,
                 wg_hbm, wu_hbm, wd_hbm, ids_hbm, gts_hbm, outb,
                 hall, xall, gn, wq, wk, wv, wo, wsg, wsu, wsd, wg, wu, wd, idg, gtg, gb, kbuf, vbuf, lens,
                 q0, q1, kn, vn, om, dense, part, rpf, rph, act, ss, sc, ps, sp, tf, ryf, xs, rxf, ty, ryo, xa, rxa, ryl,
                 lsem, wsem, ksem, vsem, osem, s_send, s_recv):
    n_rows, kvh, hd, seq, n_local, tp_size, ep_size = cfg
    d_model = hall.shape[2]
    n_chunk = n_rows // ROWS
    n_blk = n_rows // TB
    kd = kvh * hd
    tp = lax.axis_index('tp')
    ep = lax.axis_index('ep')
    partner = {'ep': ep + 1 - 2 * lax.rem(ep, 2)}
    xnbr = {'ep': lax.rem(ep + ep_size // 2, ep_size)}
    ynbr = {'tp': 1 - tp}

    def local(src, dst, sem):
        return pltpu.make_async_copy(src, dst, sem)

    n_remote = [0]

    def remote(src, dst, dev):
        i = n_remote[0]
        n_remote[0] += 1
        return pltpu.make_async_remote_copy(src_ref=src, dst_ref=dst, send_sem=s_send.at[i], recv_sem=s_recv.at[i],
                                            device_id=dev, device_id_type=pl.DeviceIdType.MESH)

    def rows(i):
        return pl.ds(i * ROWS, ROWS)

    def mine(s):
        r0, n = SUBS[s]
        return pl.ds(pl.multiple_of(r0 + tp * (n // 2), n // 2), n // 2)

    def theirs(s):
        r0, n = SUBS[s]
        return pl.ds(pl.multiple_of(r0 + (1 - tp) * (n // 2), n // 2), n // 2)

    def packed(s):
        r0, n = SUBS[s]
        return pl.ds(r0 // 2, n // 2)

    hid_cp = [local(hid_hbm, hall.at[0], lsem.at[0])]
    small_cp = [local(ids_hbm, idg.at[0], lsem.at[1]), local(gts_hbm, gtg.at[0], lsem.at[2]),
                local(gn_hbm, gn, lsem.at[3]), local(len_hbm, lens, lsem.at[4])]
    qkv_cp = [local(wq_hbm, wq, lsem.at[5]), local(wk_hbm, wk, lsem.at[6]), local(wv_hbm, wv, lsem.at[7])]
    sh_cp = [local(wsg_hbm, wsg, lsem.at[8]), local(wsu_hbm, wsu, lsem.at[9]), local(wsd_hbm, wsd, lsem.at[10]),
             *[local(wo_hbm.at[pl.ds((h * 2 + g) * hd, hd)], wo.at[pl.ds((g * kvh + h) * hd, hd)], osem.at[len(SUBS) + g * kvh + h])
               for g in range(2) for h in range(kvh)]]
    exp_cp = [local(wg_hbm, wg, wsem.at[0]), local(wu_hbm, wu, wsem.at[1]), local(wd_hbm, wd, wsem.at[2])]

    def k_cp(b):
        slot = lax.rem(b, SLOTS)
        return local(k_hbm.at[pl.ds(b * TB, TB)], kbuf.at[slot], ksem.at[slot])

    def v_cp(b):
        slot = lax.rem(b, SLOTS)
        return local(v_hbm.at[pl.ds(b * TB, TB)], vbuf.at[slot], vsem.at[slot])

    for c in hid_cp + small_cp + qkv_cp:
        c.start()
    for b in range(EARLY):
        k_cp(b).start()
        v_cp(b).start()
    for c in exp_cp:
        c.start()
    for b in range(EARLY, SLOTS):
        k_cp(b).start()
        v_cp(b).start()
    for c in sh_cp:
        c.start()

    barrier = pltpu.get_barrier_semaphore()
    for dev in (partner, xnbr, ynbr):
        pl.semaphore_signal(barrier, inc=1, device_id=dev, device_id_type=pl.DeviceIdType.MESH)
    pl.semaphore_wait(barrier, 3)

    def whole(s):
        return pl.ds(*SUBS[s])

    chunks = range(n_chunk)
    subs = range(len(SUBS))

    def sub_of(i):
        return [s for s in subs if SUBS[s][0] // ROWS == i]

    x_hid = [remote(hall.at[0, rows(i)], hall.at[2, rows(i)], xnbr) for i in chunks]
    p_hid = [remote(hall.at[0, rows(i)], hall.at[1, rows(i)], partner) for i in chunks]
    f_hid = [remote(hall.at[2, rows(i)], hall.at[3, rows(i)], partner) for i in chunks]
    x_idg = [remote(idg.at[0], idg.at[2], xnbr), remote(gtg.at[0], gtg.at[2], xnbr)]
    p_idg = [remote(idg.at[0], idg.at[1], partner), remote(gtg.at[0], gtg.at[1], partner)]
    f_idg = [remote(idg.at[2], idg.at[3], partner), remote(gtg.at[2], gtg.at[3], partner)]
    c_far = [remote(part.at[3, rows(i)], rpf.at[rows(i)], partner) for i in chunks]
    c_near = [remote(part.at[1, rows(i)], rph.at[rows(i)], partner) for i in chunks]
    def packed2(s):
        return pl.ds(first.index(s) * SUBS[s][1], SUBS[s][1])

    first, last, ends = [1, 2], subs[-1], subs[3:]
    far_subs = [s for s in subs if s not in first]
    x_all = {s: remote(xa.at[packed2(s)], rxa.at[packed2(s)], xnbr) for s in first}
    def end_rows(s):
        return pl.ds(SUBS[s][0] - SUBS[ends[0]][0], SUBS[s][1])

    y_last = {s: remote(dense.at[whole(s)], ryl.at[end_rows(s)], ynbr) for s in ends}
    y_far = {s: remote(tf.at[packed(s)], ryf.at[packed(s)], ynbr) for s in far_subs}
    x_ret = {s: remote(xs.at[packed(s)], rxf.at[packed(s)], xnbr) for s in far_subs}
    y_own = [remote(ty.at[packed(s)], ryo.at[packed(s)], ynbr) for s in subs[:3]]
    y_out = [remote(outb.at[mine(s)], outb.at[mine(s)], ynbr) for s in subs[:3]]

    for c in small_cp:
        c.wait()
    for c in x_idg + p_idg:
        c.start()
    for c in hid_cp:
        c.wait()
    for c in x_hid + p_hid:
        c.start()

    def normalize(grp, r0, n):
        def body(j, carry):
            for k in range(4):
                at = pl.ds(pl.multiple_of(r0 + j * 128 + k * 32, 32), 32)
                h32 = hall[grp, at, :].astype(F32)
                inv = lax.rsqrt(jnp.mean(h32 * h32, axis=-1, keepdims=True) + RMS_EPS)
                xall[grp, at, :] = (h32 * inv * gn[...]).astype(BF)
            return carry
        lax.fori_loop(0, n // 128, body, 0)

    first_exp = (ep * tp_size + tp) * n_local

    def gate_table(grp):
        ids = idg[grp]
        vals = gtg[grp]
        picked = [jnp.sum(jnp.where(ids == first_exp + e, vals, 0.0), axis=0, keepdims=True) for e in range(n_local)]
        table = jnp.concatenate(picked + [jnp.zeros((LANES - n_local, n_rows), F32)], axis=0)
        cols = jnp.transpose(table)
        for e in range(n_local):
            gb[grp, e] = jnp.broadcast_to(cols[:, e:e + 1], (n_rows, LANES))

    per_tok = 2 * kvh
    R = TB * per_tok
    rr = lax.broadcasted_iota(jnp.int32, (per_tok, kd), 0)
    cc = lax.broadcasted_iota(jnp.int32, (per_tok, kd), 1)
    own = (rr % kvh) == (cc // hd)
    low = rr < kvh
    pos = lax.broadcasted_iota(jnp.int32, (per_tok, seq), 1)
    scale = hd ** -0.5

    def heads(t):
        return slice(t * per_tok, (t + 1) * per_tok)

    def spread(ref, tok):
        return jnp.broadcast_to(ref[pl.ds(tok, 1), :], (per_tok, kd))

    def stage_kv(b, p, with_v=True, with_k=True):
        for t in range(TB):
            if with_k:
                tok = b * TB + t
                q_t = jnp.where(own, jnp.where(low, spread(q0, tok), spread(q1, tok)), 0.0)
                s_t = dotf(q_t.astype(BF), kbuf[lax.rem(b, SLOTS), t])
                sc[p, heads(t), :] = jnp.where(pos < lens[tok], s_t * scale, -1e30)
                self_t = jnp.sum(q_t * spread(kn, tok), axis=-1, keepdims=True) * scale
                ss[p, heads(t), :] = jnp.broadcast_to(self_t, (per_tok, LANES))
            if with_v:
                tok = (b - 2) * TB + t
                o_t = dot_nt(ps[p, heads(t), :].astype(BF), vbuf[lax.rem(b - 2, SLOTS), t])
                o_t = o_t + jnp.concatenate([sp[p, heads(t), :]] * (kd // LANES), axis=1) * spread(vn, tok)
                om[pl.ds(pl.multiple_of(tok * per_tok, per_tok), per_tok), :] = jnp.where(own, o_t, 0.0)

    def stage_s(p):
        scores = sc[p]
        self_score = ss[p, :, 0:1]
        peak = jnp.maximum(jnp.max(scores, axis=-1, keepdims=True), self_score)
        prob = jnp.exp(scores - peak)
        self_prob = jnp.exp(self_score - peak)
        inv = 1.0 / (jnp.sum(prob, axis=-1, keepdims=True) + self_prob)
        ps[p] = prob * inv
        sp[p] = jnp.broadcast_to((self_prob * inv).astype(BF).astype(F32), (R, LANES))

    def attn_pair(j, carry):
        b = 2 * j
        for p in range(2):
            k_cp(b + p).wait()
            v_cp(b + p - 2).wait()
        for p in range(2):
            stage_kv(b + p, p)
            stage_s(1 - p)
        for p in range(2):
            @pl.when(b + p + SLOTS < n_blk)
            def _():
                k_cp(b + p + SLOTS).start()

            @pl.when(b + p - 2 + SLOTS < n_blk)
            def _():
                v_cp(b + p - 2 + SLOTS).start()
        return carry

    done = [0]

    def attend(hi):
        lo = done[0]
        done[0] = hi
        if lo == 0:
            for p in range(2):
                k_cp(p).wait()
            for p in range(2):
                stage_kv(p, p, with_v=False)
            stage_s(0)
            for p in range(2):
                k_cp(p + SLOTS).start()
            lo = 2
        lax.fori_loop(lo // 2, hi // 2, attn_pair, 0)

    def attend_last():
        for p in range(2):
            v_cp(n_blk - 2 + p).wait()
        stage_kv(n_blk, 0, with_k=False)
        stage_s(1)
        stage_kv(n_blk + 1, 1, with_k=False)

    ff = wg.shape[2]

    def unit(g0, r0, n):
        at = pl.ds(r0, n)
        m2 = 2 * n

        xr = xall[g0:g0 + 2, at, :].reshape(m2, d_model)

        def up(e, j):
            cs = slice(j * 256, (j + 1) * 256)
            g_a = dotf(xr, wg[e, :, cs])
            u_b = dotf(xr, wu[e, :, cs])
            act[e % 2, :, cs] = (g_a * jax.nn.sigmoid(g_a) * u_b).astype(BF)

        def down(e, j):
            gate = gb[g0:g0 + 2, e, at, :].reshape(m2, LANES)
            y = dotf(act[e % 2], wd[e, :, j * 256:(j + 1) * 256]).astype(BF).astype(F32)
            for m in range(256 // LANES):
                ls = slice(j * 256 + m * LANES, j * 256 + (m + 1) * LANES)
                add = jnp.where(gate > 0.0, gate * y[:, m * LANES:(m + 1) * LANES], 0.0).reshape(2, n, LANES)
                part[g0:g0 + 2, at, ls] = add if e == 0 else part[g0:g0 + 2, at, ls] + add

        n_up = ff // 256
        n_down = d_model // 256
        for e in range(n_local + 1):
            for j in range(n_up):
                if e < n_local:
                    up(e, j)
                if e > 0:
                    for k in range(j * n_down // n_up, (j + 1) * n_down // n_up):
                        down(e - 1, k)

    def far_send(i):
        c_far[i].wait_recv()
        for s in sub_of(i)[::-1]:
            if s in first:
                at = whole(s)
                xa[packed2(s), :] = part[2, at, :] + rpf[at, :]
                x_all[s].start()
            else:
                at = theirs(s)
                tf[packed(s), :] = part[2, at, :] + rpf[at, :]
                y_far[s].start()

    def far_x(some):
        for s in some:
            y_far[s].wait_recv()
            at = mine(s)
            xs[packed(s), :] = part[2, at, :] + rpf[at, :] + ryf[packed(s), :]
            x_ret[s].start()

    def arrive(i):
        x_hid[i].wait_recv()
        f_hid[i].start()
        normalize(2, i * ROWS, ROWS)

    def far(i):
        f_hid[i].wait_recv()
        normalize(3, i * ROWS, ROWS)
        unit(2, i * ROWS, ROWS)
        c_far[i].start()

    def near(i):
        p_hid[i].wait_recv()
        normalize(1, i * ROWS, ROWS)
        unit(0, i * ROWS, ROWS)
        c_near[i].start()

    def shared_expert():
        for c in sh_cp:
            c.wait()
        sg = dotf(xall[0], wsg[...])
        su = dotf(xall[0], wsu[...])
        sa = (sg * jax.nn.sigmoid(sg) * su).astype(BF)
        for j in range(d_model // 256):
            cs = slice(j * 256, (j + 1) * 256)
            dense[:, cs] = dotf(sa, wsd[:, cs])

    def own_y(s):
        r0, n = SUBS[s]
        if s in (sub_of(0)[0], sub_of(1)[0]):
            c_near[r0 // ROWS].wait_recv()
        at = pl.ds(r0, n)
        gather_o = one_hot_mat(2 * n, n * per_tok, lambda r, c: (c // per_tok == r % n) & ((c % per_tok) // kvh == r // n))
        o2 = dotf(gather_o, om[pl.ds(r0 * per_tok, n * per_tok), :].astype(BF)).astype(BF)
        ctx_bf = jnp.concatenate([o2[0:n], o2[n:2 * n]], axis=1)
        if s in first:
            x_all[s].wait_recv()
        for j in range(d_model // 256):
            cs = slice(j * 256, (j + 1) * 256)
            total = dense[at, cs] + dotf(ctx_bf, wo[:, cs]) + part[0, at, cs] + rph[at, cs]
            dense[at, cs] = total + rxa[packed2(s), cs] if s in first else total
        if s in ends:
            x_ret[s].wait_recv()
            dense[mine(s), :] = dense[mine(s), :] + rxf[packed(s), :]
            y_last[s].start()
        else:
            ty[packed(s), :] = dense[theirs(s), :]
            y_own[s].start()

    def finish(s):
        if s in ends:
            at = whole(s)
            y_last[s].wait_recv()
            outb[at, :] = (hall[0, at, :].astype(F32) + (dense[at, :] + ryl[end_rows(s), :])).astype(BF)
            return
        at = mine(s)
        y_own[s].wait_recv()
        total = dense[at, :] + ryo[packed(s), :]
        if s in far_subs:
            x_ret[s].wait_recv()
            total = total + rxf[packed(s), :]
        outb[at, :] = (hall[0, at, :].astype(F32) + total).astype(BF)
        y_out[s].start()

    normalize(0, 0, n_rows)
    for c in qkv_cp:
        c.wait()

    nq = wq.shape[1]
    q_bf = [dotf(xall[0], wq[:, j * 256:(j + 1) * 256]).astype(BF) for j in range(nq // 256)]
    for g, ref in enumerate((q0, q1)):
        acc = None
        for j in range(nq // 256):
            def sel(r, c, j=j, g=g):
                r2 = r + j * 256
                return ((r2 // (2 * hd)) == (c // hd)) & ((r2 % (2 * hd)) == g * hd + c % hd)
            term = dotf(q_bf[j], one_hot_mat(256, kd, sel))
            acc = term if acc is None else acc + term
        ref[...] = acc
    kn[...] = dotf(xall[0], wk[...]).astype(BF).astype(F32)
    vn[...] = dotf(xall[0], wv[...]).astype(BF).astype(F32)

    attend(6)
    for c in p_idg + x_idg:
        c.wait_recv()
    for c in f_idg:
        c.start()
    gate_table(0)
    gate_table(1)
    gate_table(2)
    for c in exp_cp:
        c.wait()
    near(0)
    arrive(0)
    attend(8)
    for c in f_idg:
        c.wait_recv()
    gate_table(3)
    far(0)
    arrive(1)
    attend(12)
    far_send(0)
    far(1)
    shared_expert()
    own_y(0)
    attend(14)
    far_send(1)
    attend(16)
    far_x([0])
    attend(18)
    own_y(1)
    near(1)
    attend(22)
    far_x([5, 4, 3])
    attend(26)
    finish(0)
    own_y(2)
    attend(30)
    own_y(3)
    finish(1)
    attend(n_blk)
    own_y(4)
    attend_last()
    own_y(5)
    finish(2)
    finish(3)
    finish(4)
    finish(5)
    for s in subs:
        if s not in ends:
            y_out[s].wait_recv()
    for c in x_hid + p_hid + f_hid + x_idg + p_idg + f_idg + c_far + c_near + list(x_all.values()) + list(y_far.values()) + list(x_ret.values()) + y_own + y_out + list(y_last.values()):
        c.wait_send()


def solution(mesh):
    tp_size = mesh.shape['tp']
    ep_size = mesh.shape['ep']
    tok_spec = P(('rep', 'ep'), None)
    col_spec = P(None, 'tp')
    row_spec = P('tp', None)
    cache_spec = P(('rep', 'ep'), None, 'tp', None)
    expert_spec = P(('ep', 'tp'), None, None)

    def device_step(hidden, g_norm, w_q, w_k, w_v, w_o, k_cache, v_cache, lengths, w_sh_gate, w_sh_up, w_sh_down, w_gate, w_up, w_down, expert_ids, gate_vals):
        n_rows, d = hidden.shape
        _, seq, kvh, hd = k_cache.shape
        n_local, _, ff = w_gate.shape
        fs = w_sh_gate.shape[1]
        kd = kvh * hd
        top = expert_ids.shape[1]
        k_t = k_cache.transpose(0, 2, 3, 1).reshape(n_rows, kd, seq)
        v_t = v_cache.transpose(0, 2, 3, 1).reshape(n_rows, kd, seq)
        cfg = (n_rows, kvh, hd, seq, n_local, tp_size, ep_size)
        n_chunk = n_rows // ROWS
        n_sub = len(SUBS)
        n_remote = 5 * n_chunk + 6 + 4 * n_sub
        R = TB * 2 * kvh
        args = (hidden, g_norm.reshape(1, d), w_q, w_k, w_v, w_o, k_t, v_t, lengths, w_sh_gate, w_sh_up, w_sh_down,
                w_gate, w_up, w_down, expert_ids.T, gate_vals.T)
        v = pltpu.VMEM
        dma = pltpu.SemaphoreType.DMA
        scratch = [
            v((4, n_rows, d), BF), v((4, n_rows, d), BF), v((1, d), F32), v(w_q.shape, BF), v(w_k.shape, BF), v(w_v.shape, BF), v(w_o.shape, BF),
            v(w_sh_gate.shape, BF), v(w_sh_up.shape, BF), v(w_sh_down.shape, BF), v(w_gate.shape, BF), v(w_up.shape, BF), v(w_down.shape, BF),
            v((4, top, n_rows), jnp.int32), v((4, top, n_rows), F32), v((4, n_local, n_rows, LANES), F32),
            v((SLOTS, TB, kd, seq), BF), v((SLOTS, TB, kd, seq), BF), pltpu.SMEM((n_rows,), jnp.int32),
            v((n_rows, kd), F32), v((n_rows, kd), F32), v((n_rows, kd), F32), v((n_rows, kd), F32), v((n_rows * 2 * kvh, kd), F32),
            v((n_rows, d), F32), v((4, n_rows, d), F32), v((n_rows, d), F32), v((n_rows, d), F32), v((2, 2 * ROWS, ff), BF),
            v((2, R, LANES), F32), v((2, R, seq), F32), v((2, R, seq), F32), v((2, R, LANES), F32),
            *[v((n_rows // 2, d), F32)] * 6, v((ROWS, d), F32), v((ROWS, d), F32), v((sum(n for _, n in SUBS[3:]), d), F32),
            dma((12,)), dma((3,)), dma((SLOTS,)), dma((SLOTS,)), dma((n_sub + 2 * kvh,)), dma((n_remote,)), dma((n_remote,)),
        ]
        return pl.pallas_call(
            functools.partial(layer_kernel, cfg),
            out_shape=pltpu.VMEM((n_rows, d), BF),
            in_specs=[pl.BlockSpec(memory_space=pl.ANY)] * len(args),
            out_specs=pl.BlockSpec(memory_space=pltpu.VMEM),
            scratch_shapes=scratch,
            compiler_params=pltpu.CompilerParams(collective_id=0, has_side_effects=True, vmem_limit_bytes=62 * 2**20),
            name='layer',
        )(*args)

    return jax.shard_map(device_step, mesh=mesh, in_specs=(tok_spec, P(None), col_spec, col_spec, col_spec, row_spec, cache_spec, cache_spec, P(('rep', 'ep')), col_spec, col_spec, row_spec, expert_spec, expert_spec, expert_spec, tok_spec, tok_spec), out_specs=tok_spec, check_vma=False)
```
